512 devices in a mesh: seq: 32 (over y_lo, z), head: 16 (over y_hi, x, core).
Axes of the slice: x: 4, y: 8 (y_hi: 2, y_lo: 4; y = y_hi * 4 + y_lo), z: 8, core: 2. Of those that a mesh axis runs over, the one named last changes fastest.
Arguments:
- tokens: bfloat16 [4096, 2560], P('seq'), may hold values from -51 to 51
- raw_keys: bfloat16 [131072, 768], P(('seq', 'head')), may hold values from -6 to 6
- raw_values: bfloat16 [131072, 512], P(('seq', 'head')), may hold values from -6 to 6
- query_weight: bfloat16 [2560, 12288], P('seq', 'head'), may hold values from -0.125 to 0.125
- output_weight: bfloat16 [8192, 2560], P('head', 'seq'), may hold values from -0.125 to 0.125
- key_expand: bfloat16 [192, 768], replicated, may hold values from -0.4375 to 0.4375
- key_mix: float32 [32, 768], replicated, may hold values from -1 to 1
- key_reduce: bfloat16 [768, 192], replicated, may hold values from -1.6953125 to 1.6953125
- value_expand: bfloat16 [128, 768], replicated, may hold values from -0.5 to 0.5
- value_mix: float32 [32, 768], replicated, may hold values from -1 to 1
- value_reduce: bfloat16 [768, 128], replicated, may hold values from -0.65625 to 0.65625
Outputs:
- branch_output: bfloat16 [4096, 2560], P('seq', 'head')
The draws below stay inside these ranges and needn't reach their ends.
All inputs are finite; a program needn't handle non-finite values.
Results may differ from the reference program's by a relative error of at most 0.008.
The reference program's roundings to bfloat16 on the way count: a program that leaves them out, or rounds other values in their place, can miss the bound.
Values may be sent and summed in bfloat16 or wider, within the bound.
A program may use at most 64 MiB of HBM per device.

```python
import jax
import jax.numpy as jnp
from jax import lax

D = 2560
H = 64
G = 4
DK = 192
DV = 128
BLK = 32
STRIDE = 16
HID = 768
NEW = 4096
CTX = 126976
TOTAL = 131072
NB = 8192


def draw_tokens(key, part):
    base_key = jax.random.fold_in(jax.random.fold_in(key, 11), 0)
    return jnp.clip(jax.random.normal(base_key, (NEW, D), jnp.float32), -6.0, 6.0).astype(jnp.bfloat16)


def with_spikes(drawn, own_key, source, target, parts, factor):
    owner, partner = [(jnp.arange(drawn.shape[position]) // (drawn.shape[position] // parts)).reshape([-1 if axis == position else 1 for axis in range(drawn.ndim)]) for position in (source, target)]
    chosen = jax.random.permutation(own_key, parts)[partner]
    strong = (owner == chosen) | (owner == (partner + parts // 2) % parts)
    return jnp.where(strong, factor * drawn, drawn)


def block_levels(stream_key, shape, shards, smallest, high):
    gain, own = 1.0, jax.random.fold_in(stream_key, 6)
    for dim, shards_of in shards:
        heights = jnp.exp(jax.random.uniform(jax.random.fold_in(own, dim), (shards_of,), jnp.float32, smallest / len(shards), high / len(shards)))
        gain = gain * jnp.repeat(heights, shape[dim] // shards_of).reshape([-1 if axis == dim else 1 for axis in range(len(shape))])
    return gain


def gaussian(own_key, extent, deviation, reach, shards=(), kind=jnp.bfloat16):
    loudness = block_levels(own_key, extent, shards, -0.22, 0.18) if shards else 1.0
    result = jax.random.normal(own_key, extent, jnp.float32) * deviation * loudness
    return jnp.minimum(jnp.maximum(result, -reach), reach).astype(kind)


def gaussian_with(own_key, extent, width, reach, shards, heavy, kind=jnp.bfloat16):
    result = width * jax.random.normal(own_key, extent, jnp.float32)
    if shards:
        result = result * block_levels(own_key, extent, shards, -0.22, 0.18)
    return jnp.clip(with_spikes(result, jax.random.fold_in(own_key, 3), *heavy), -reach, reach).astype(kind)


def setup_inputs(seed: int = 0) -> dict:
    key_of = jax.random.split(jax.random.key(seed), 12)
    tokens = draw_tokens(jax.random.fold_in(key_of[11], 71), 0)
    raw_keys = gaussian(key_of[1], (TOTAL, G * DK), 1.0, 6.0, ((0, 512),))
    raw_values = gaussian(key_of[2], (TOTAL, G * DV), 1.0, 6.0, ((0, 512),))
    query_weight = gaussian(key_of[3], (D, H * DK), D ** -0.5, 0.125, ((0, 32), (1, 16)))
    output_weight = gaussian_with(key_of[4], (H * DV, D), (H * DV) ** -0.5, 0.125, ((0, 16), (1, 32)), (0, 1, 32, 2.75))
    key_expand = gaussian(key_of[5], (DK, HID), DK ** -0.5, 0.4375)
    key_mix = gaussian(key_of[6], (BLK, HID), BLK ** -0.5, 1.0, (), jnp.float32)
    key_reduce = gaussian(key_of[7], (HID, DK), 0.28, 1.6953125)
    value_expand = gaussian(key_of[8], (DV, HID), DV ** -0.5, 0.5)
    value_mix = gaussian(key_of[9], (BLK, HID), BLK ** -0.5, 1.0, (), jnp.float32)
    value_reduce = gaussian(key_of[10], (HID, DV), 0.11, 0.65625)
    return dict(tokens=tokens, raw_keys=raw_keys, raw_values=raw_values, query_weight=query_weight, output_weight=output_weight, key_expand=key_expand, key_mix=key_mix, key_reduce=key_reduce, value_expand=value_expand, value_mix=value_mix, value_reduce=value_reduce)


def compress(raw, expand, position_mix, reduce_weight):
    width_in = expand.shape[0]
    compressed_list = []
    for group in range(G):
        group_tokens = raw[:, group * width_in:(group + 1) * width_in]
        projected = jnp.dot(group_tokens, expand, preferred_element_type=jnp.float32)
        projected = jnp.concatenate([projected, jnp.zeros((STRIDE, projected.shape[1]), jnp.float32)], axis=0)
        projected = projected.reshape(NB + 1, STRIDE, projected.shape[1])
        hidden = jnp.sum(projected[:-1] * position_mix[:STRIDE][None], axis=1)
        hidden = hidden + jnp.sum(projected[1:] * position_mix[STRIDE:][None], axis=1)
        activated = jax.nn.gelu(hidden, approximate=False).astype(jnp.bfloat16)
        compressed_list.append(jnp.dot(activated, reduce_weight, preferred_element_type=jnp.float32).astype(jnp.bfloat16))
    return jnp.stack(compressed_list)


def reference(tokens, raw_keys, raw_values, query_weight, output_weight, key_expand, key_mix, key_reduce, value_expand, value_mix, value_reduce):
    packed_keys = compress(raw_keys, key_expand, key_mix, key_reduce)
    packed_values = compress(raw_values, value_expand, value_mix, value_reduce)
    queries = jnp.dot(tokens, query_weight, preferred_element_type=jnp.float32).astype(jnp.bfloat16)
    queries = queries.reshape(NEW, H, DK).transpose(1, 0, 2)
    positions = CTX + jnp.arange(NEW, dtype=jnp.int32)
    block_index = jnp.arange(NB, dtype=jnp.int32)
    visible = (STRIDE * block_index + BLK - 1)[None, :] <= positions[:, None]
    score_scale = DK ** -0.5

    def one_head(inputs):
        head_queries, head_index = inputs
        group = head_index // (H // G)
        keys_group = lax.dynamic_index_in_dim(packed_keys, group, 0, keepdims=False)
        values_group = lax.dynamic_index_in_dim(packed_values, group, 0, keepdims=False)
        scores = jnp.dot(head_queries, keys_group.T, preferred_element_type=jnp.float32) * score_scale
        scores = jnp.where(visible, scores, -jnp.inf)
        row_max = jnp.max(scores, axis=1, keepdims=True)
        exponent = jnp.exp(scores - row_max)
        row_total = jnp.sum(exponent, axis=1, keepdims=True)
        numerator = jnp.dot(exponent.astype(jnp.bfloat16), values_group, preferred_element_type=jnp.float32)
        return (numerator / row_total).astype(jnp.bfloat16)

    attended = lax.map(one_head, (queries, jnp.arange(H, dtype=jnp.int32)))
    attended = attended.transpose(1, 0, 2).reshape(NEW, H * DV)
    return jnp.dot(attended, output_weight, preferred_element_type=jnp.float32).astype(jnp.bfloat16)
```

```python
import functools

import jax
import jax.numpy as jnp
from jax import lax
from jax.experimental import pallas as pl
from jax.experimental.pallas import tpu as pltpu
from jax.sharding import PartitionSpec as P

G = 4
BLK = 32
STRIDE = 16
CTX = 126976
DK = 192
DV = 128
KV_WIDTH = 384
SEQ_HEAD = ("seq", "head")
MESH = pl.DeviceIdType.MESH
BF16 = jnp.bfloat16
F32 = jnp.float32
EXP2_SCALE = DK**-0.5 * 1.4426950408889634


def shifted(block, axis, distance):
    devices = range(lax.axis_size(axis))
    route = [(i - distance, i) for i in devices if i - distance in devices]
    return lax.ppermute(block, axis, route)


def project(raw, expand, groups):
    width_in = expand.shape[0]
    shaped = raw.reshape(raw.shape[0], groups, width_in)
    return jnp.einsum("tgc,ch->tgh", shaped, expand, preferred_element_type=F32)


def half_sums(projected, mix_half):
    shaped = projected.reshape(-1, STRIDE, projected.shape[1], projected.shape[2])
    return jnp.sum(shaped * mix_half[None, :, None, :], axis=1)


def finish(hidden, reduce_weight):
    activated = jax.nn.gelu(hidden, approximate=False).astype(BF16)
    return jnp.einsum(
        "bgh,hc->gbc", activated, reduce_weight, preferred_element_type=F32
    ).astype(BF16)


def compress(raw_keys, raw_values, key_expand, key_mix, key_reduce, value_expand, value_mix, value_reduce):
    key_proj = project(raw_keys, key_expand, G)
    value_proj = project(raw_values, value_expand, G)
    tail_keys = jnp.sum(key_proj[:STRIDE] * key_mix[STRIDE:][:, None, :], axis=0)
    tail_values = jnp.sum(value_proj[:STRIDE] * value_mix[STRIDE:][:, None, :], axis=0)
    edge_keys, edge_values = shifted((tail_keys, tail_values), SEQ_HEAD, -1)
    later_keys = jnp.concatenate(
        [half_sums(key_proj[STRIDE:], key_mix[STRIDE:]), edge_keys[None]], axis=0
    )
    later_values = jnp.concatenate(
        [half_sums(value_proj[STRIDE:], value_mix[STRIDE:]), edge_values[None]], axis=0
    )
    hidden_keys = half_sums(key_proj, key_mix[:STRIDE]) + later_keys
    hidden_values = half_sums(value_proj, value_mix[:STRIDE]) + later_values
    packed_keys = finish(hidden_keys, key_reduce)
    packed_values = finish(hidden_values, value_reduce)
    pad = jnp.zeros((G, packed_keys.shape[1], KV_WIDTH - DK - DV), BF16)
    return jnp.concatenate([packed_keys, pad, packed_values], axis=2)


class Place:
    def __init__(self):
        self.s = s = lax.axis_index("seq")
        self.h = h = lax.axis_index("head")
        self.y, self.z = s // 8, s % 8
        self.g, self.j = h // 4, h % 4
        self.core = h % 2
        self.x = (h // 2) % 4
        self.y_hi = h // 8
        self.parity = self.y % 2
        self.seq_pair = (self.y + 1 - 2 * self.parity) * 8 + self.z
        self.mate = h + 1 - 2 * self.core
        self.head_pair = h + 2 - 4 * ((h // 2) % 2)
        self.head_far = (h + 8) % 16
        self.right = self.y * 8 + (self.z + 1) % 8
        self.left = self.y * 8 + (self.z + 7) % 8

    def seq_at(self, y):
        return y * 8 + self.z


def remote(src, dst, send_sem, recv_sem, seq, head):
    return pltpu.make_async_remote_copy(
        src_ref=src,
        dst_ref=dst,
        send_sem=send_sem,
        recv_sem=recv_sem,
        device_id=(seq, head),
        device_id_type=MESH,
    )


class Gather:
    def __init__(self, at, buf, rows, sems):
        self.at, self.buf, self.rows = at, buf, rows
        self.ys, self.yr, self.zs, self.zr = sems
        self.started = []

    def piece(self, i, z):
        start = pl.multiple_of(self.rows * z, 16)
        return self.buf.at[i, pl.ds(start, self.rows), :]

    def pair(self, stream, z):
        start = pl.multiple_of(self.rows * z, 16)
        return self.buf.at[pl.ds(2 * stream, 2), pl.ds(start, self.rows), :]

    def y_copy(self, i, source):
        at = self.at
        target = (at.y + 4 - i) % 4
        return remote(
            source(target), self.piece(i, at.z), self.ys.at[i], self.yr.at[i], at.seq_at(target), at.h
        )

    def start_y(self, source):
        for i in (1, 2, 3):
            copy = self.y_copy(i, source)
            copy.start()
            self.started.append(copy)

    def wait_y(self, i, source):
        self.y_copy(i, source).wait_recv()

    def z_copy(self, way, stream, step, z):
        at = self.at
        block = self.pair(stream, z)
        return remote(
            block,
            block,
            self.zs.at[way, stream, step - 1],
            self.zr.at[way, stream, step - 1],
            (at.right, at.left)[way],
            at.h,
        )

    def ways(self, stream, step):
        return (0, 1) if step < 4 else (stream,)

    def send_z(self, stream, step):
        at = self.at
        for way in self.ways(stream, step):
            z = (at.z + 8 - (step - 1)) % 8 if way == 0 else (at.z + step - 1) % 8
            copy = self.z_copy(way, stream, step, z)
            copy.start()
            self.started.append(copy)

    def came_from(self, way, step):
        at = self.at
        return (at.z + 8 - step) % 8 if way == 0 else (at.z + step) % 8

    def wait_z(self, stream, step):
        for way in self.ways(stream, step):
            self.z_copy(way, stream, step, self.came_from(way, step)).wait_recv()

    def finish_sends(self):
        for copy in self.started:
            copy.wait_send()


def attend_half(who, at, qbuf, stacked, kvb, scores, lane_max, store):
    for half in range(2):
        for head in range(2):
            rows = pl.ds((2 * half + head) * 128, 128)
            stacked[rows, 0:DK] = qbuf[who, half, :, head * DK : (head + 1) * DK]
    lane_max[...] = jnp.full_like(lane_max, -jnp.inf)
    last = (3 + 4 - at.y) % 4
    first_position = CTX + at.s * 128
    half_index = (at.h // 2) % 2

    def score_chunk(chunk, carry):
        keys = kvb[chunk // 4, chunk % 4, :, 0:256]
        block = lax.dot_general(
            stacked[...], keys, (((1,), (1,)), ((), ())), preferred_element_type=F32
        )
        scores[chunk] = block

        @pl.when(chunk % 4 == last)
        def _():
            tail = scores[chunk, :, 384:512]
            column = lax.broadcasted_iota(jnp.int32, tail.shape, 1)
            row = lax.broadcasted_iota(jnp.int32, tail.shape, 0) % 128
            ids = 256 * (30 + column // 64) + 64 * (2 * half_index + chunk // 4) + column % 64
            visible = STRIDE * ids + BLK - 1 <= first_position + row
            scores[chunk, :, 384:512] = jnp.where(visible, tail, -jnp.inf)

        top = lane_max[...]
        for k in range(4):
            top = jnp.maximum(top, scores[chunk, :, 128 * k : 128 * (k + 1)])
        lane_max[...] = top
        return carry

    lax.fori_loop(0, 8, score_chunk, 0)

    for head in range(4):
        rows = slice(head * 128, (head + 1) * 128)
        row_max = jnp.max(lane_max[rows, :], axis=1, keepdims=True)

        def weigh_chunk(chunk, carry):
            total, numerator = carry
            exponent = jnp.exp2((scores[chunk, rows, :] - row_max) * EXP2_SCALE)
            for k in range(4):
                total = total + exponent[:, 128 * k : 128 * (k + 1)]
            values = kvb[chunk // 4, chunk % 4, :, 256:384]
            numerator = numerator + jnp.dot(
                exponent.astype(BF16), values, preferred_element_type=F32
            )
            return total, numerator

        start = jnp.zeros((128, 128), F32)
        total, numerator = lax.fori_loop(0, 8, weigh_chunk, (start, start))
        row_total = jnp.sum(total, axis=1, keepdims=True)
        store(head, row_max, row_total, numerator)


def kernel(
    tokens,
    kv4,
    qw,
    ow,
    out,
    qwb,
    owb,
    kvb,
    tokp,
    qbuf,
    qother,
    stacked,
    scores,
    lane_max,
    mine,
    mine_max,
    mine_total,
    part,
    stats,
    part_in,
    stats_in,
    attended,
    summed,
    o1,
    o1_in,
    o2,
    o2_in,
    o3,
    o3_in,
    q_ys, q_yr, q_zs, q_zr,
    k_ys, k_yr, k_zs, k_zr,
    o_ys, o_yr, o_zs, o_zr,
    r_s, r_r,
    m_s, m_r,
    e_s, e_r,
):
    at = Place()
    s, h, c = at.s, at.h, at.core

    barrier = pltpu.get_barrier_semaphore()
    partners = [(s, (h + d) % 16) for d in range(1, 16)]
    partners += [(at.seq_at((at.y + d) % 4), h) for d in (1, 2, 3)]
    partners += [(at.right, h), (at.left, h), (at.seq_pair, at.head_pair)]
    for partner in partners:
        pl.semaphore_signal(barrier, inc=1, device_id=partner, device_id_type=MESH)
    pl.semaphore_wait(barrier, len(partners))

    started = []

    def go(copy):
        copy.start()
        started.append(copy)
        return copy

    q = Gather(at, qwb, 80, (q_ys, q_yr, q_zs, q_zr))
    o = Gather(at, owb, 80, (o_ys, o_yr, o_zs, o_zr))
    k = Gather(at, kvb.at[c], 64, (k_ys, k_yr, k_zs, k_zr))

    own_rows = pl.ds(pl.multiple_of(64 * at.z + 16 * at.j, 16), 16)

    def spread_copy(group):
        quarter = at.g % 2
        return remote(
            kv4.at[group],
            kvb.at[quarter, 0, own_rows, :],
            r_s.at[group],
            r_r.at[at.j],
            s,
            4 * group + at.g,
        )

    for group in range(G):
        @pl.when(4 * group + at.g != h)
        def _(group=group):
            spread_copy(group).start()

        @pl.when(4 * group + at.g == h)
        def _(group=group):
            kvb[c, 0, own_rows, :] = kv4[group]

    def q_source(target):
        return qw.at[:, pl.ds(pl.multiple_of(384 * (target % 2), 128), 384)]

    q.start_y(q_source)
    qwb[0, pl.ds(pl.multiple_of(80 * at.z, 16), 80), :] = qw[
        :, pl.ds(pl.multiple_of(384 * at.parity, 128), 384)
    ]
    tok_copy = go(remote(tokens, tokp, e_s.at[0], e_r.at[0], at.seq_pair, h))
    q.wait_y(1, q_source)
    q.send_z(0, 1)
    q.wait_y(2, q_source)
    q.wait_y(3, q_source)
    q.send_z(1, 1)

    for m in range(4):
        @pl.when(4 * at.j + m != h)
        def _(m=m):
            rows = pl.ds(pl.multiple_of(64 * at.z + 16 * m, 16), 16)
            remote(
                kv4.at[0], kvb.at[c, 0, rows, :], r_s.at[0], r_r.at[m], s, 4 * at.j + m
            ).wait_recv()

    def k_source(target):
        return k.piece(0, at.z)

    k.start_y(k_source)

    def mate_copy(quarter, stream, index, z):
        start = pl.multiple_of(64 * z, 16)
        block = kvb.at[quarter, pl.ds(2 * stream, 2), pl.ds(start, 64), :]
        return remote(
            block, block, m_s.at[stream, index], m_r.at[stream, index], s, at.mate
        )

    def k_arrived(stream, step):
        k.wait_z(stream, step)
        for way in k.ways(stream, step):
            index = 7 if step == 4 else 3 * way + step
            go(mate_copy(c, stream, index, k.came_from(way, step)))

    def q_round(step):
        for stream in (0, 1):
            q.wait_z(stream, step - 1)
            q.send_z(stream, step)

    def k_round(step):
        for stream in (0, 1):
            k_arrived(stream, step - 1)
            k.send_z(stream, step)

    q_round(2)
    k.wait_y(1, k_source)
    k.send_z(0, 1)
    go(mate_copy(c, 0, 0, at.z))
    k.wait_y(2, k_source)
    k.wait_y(3, k_source)
    k.send_z(1, 1)
    go(mate_copy(c, 1, 0, at.z))
    ow_source = lambda target: ow
    o.start_y(ow_source)
    owb[0, pl.ds(pl.multiple_of(80 * at.z, 16), 80), :] = ow[...]
    q_round(3)
    k_round(2)
    q_round(4)
    k_round(3)
    q.wait_z(0, 4)
    q.wait_z(1, 4)
    tok_copy.wait_recv()

    def project_queries(source):
        total = jnp.zeros((128, 384), F32)
        for i in range(4):
            start = pl.multiple_of(640 * ((at.y + i) % 4), 128)
            total = total + jnp.dot(
                source[:, pl.ds(start, 640)], qwb[i], preferred_element_type=F32
            )
        return total.astype(BF16)

    qother[...] = project_queries(tokp)
    q_in = [
        remote(qother, qbuf.at[0, at.parity], e_s.at[1], e_r.at[1], at.seq_pair, h),
        remote(qother, qbuf.at[1, at.parity], e_s.at[2], e_r.at[2], at.seq_pair, at.head_pair),
    ]
    go(q_in[0])
    go(q_in[1])
    qbuf[0, at.parity] = project_queries(tokens)
    q_in.append(
        go(
            remote(
                qbuf.at[0, at.parity], qbuf.at[1, at.parity], e_s.at[3], e_r.at[3], s, at.head_pair
            )
        )
    )
    k_round(4)
    o.wait_y(1, ow_source)
    o.send_z(0, 1)
    o.wait_y(2, ow_source)
    o.wait_y(3, ow_source)
    o.send_z(1, 1)
    k_arrived(0, 4)
    k_arrived(1, 4)
    stacked[:, DK:] = jnp.zeros((512, 256 - DK), BF16)
    q_in[0].wait_recv()
    q_in[2].wait_recv()
    q_in[1].wait_recv()
    for stream in (0, 1):
        mate_copy(1 - c, stream, 0, at.z).wait_recv()
        for step in (1, 2, 3, 4):
            for way in k.ways(stream, step):
                index = 7 if step == 4 else 3 * way + step
                mate_copy(1 - c, stream, index, k.came_from(way, step)).wait_recv()

    lane = lax.broadcasted_iota(jnp.int32, (128, 128), 1)

    def store_part(head, row_max, row_total, numerator):
        part[head] = numerator.astype(BF16)
        tile = jnp.where(lane == 0, row_max, jnp.where(lane == 1, row_total, 0.0))
        stats[head] = jnp.transpose(tile)[0:8, :]

    attend_half(1, at, qbuf, stacked, kvb, scores, lane_max, store_part)
    part_copy = go(remote(part, part_in, e_s.at[4], e_r.at[4], s, at.head_pair))
    stat_copy = go(remote(stats, stats_in, e_s.at[5], e_r.at[5], s, at.head_pair))
    for stream in (0, 1):
        o.wait_z(stream, 1)
        o.send_z(stream, 2)

    def store_mine(head, row_max, row_total, numerator):
        mine[head] = numerator
        mine_max[head] = jnp.broadcast_to(row_max, (128, 128))
        mine_total[head] = jnp.broadcast_to(row_total, (128, 128))

    attend_half(0, at, qbuf, stacked, kvb, scores, lane_max, store_mine)
    for stream in (0, 1):
        o.wait_z(stream, 2)
        o.send_z(stream, 3)
    part_copy.wait_recv()
    stat_copy.wait_recv()
    for head in range(4):
        tile = jnp.concatenate([stats_in[head], jnp.zeros((120, 128), F32)], axis=0)
        tile = jnp.transpose(tile)
        other_max = jnp.broadcast_to(tile[:, 0:1], (128, 128))
        other_total = jnp.broadcast_to(tile[:, 1:2], (128, 128))
        top = jnp.maximum(mine_max[head], other_max)
        own_part = jnp.exp2((mine_max[head] - top) * EXP2_SCALE)
        other_part = jnp.exp2((other_max - top) * EXP2_SCALE)
        total = mine_total[head] * own_part + other_total * other_part
        value = mine[head] * own_part + part_in[head].astype(F32) * other_part
        attended[:, head * DV : (head + 1) * DV] = (value / total).astype(BF16)
    for stream in (0, 1):
        o.wait_z(stream, 3)
        o.send_z(stream, 4)
    o.wait_z(0, 4)
    o.wait_z(1, 4)

    for i in range(4):
        start = pl.multiple_of(4 * ((at.y + i) % 4), 4)
        block = lax.dot_general(
            owb[i], attended[...], (((1,), (1,)), ((), ())), preferred_element_type=F32
        ).reshape(2, 2, 160, 128)
        summed[pl.ds(2 * ((at.y + i) % 4), 2)] = block
        o1[pl.ds(2 * ((at.y + i) % 4), 2)] = block.astype(BF16)
    mate_sum = go(remote(o1.at[:, 1 - c], o1_in, e_s.at[6], e_r.at[6], s, at.mate))
    mate_sum.wait_recv()
    for i in range(8):
        summed[i, 0] = summed[i, c] + o1_in[i].astype(F32)
        o2[i // 4, i % 4] = summed[i, 0].astype(BF16)
    x_sums = []
    for d in (1, 2, 3):
        x = (at.x + d) % 4
        x_sums.append(
            go(
                remote(
                    o2.at[:, x], o2_in.at[d - 1], e_s.at[6 + d], e_r.at[6 + d], s, 8 * at.y_hi + 2 * x + c
                )
            )
        )
    for copy in x_sums:
        copy.wait_recv()
    far = 1 - at.y_hi
    value = summed[4 * far + at.x, 0]
    for d in range(3):
        value = value + o2_in[d, far].astype(F32)
    o3[...] = value.astype(BF16)
    y_sum = go(remote(o3, o3_in, e_s.at[10], e_r.at[10], s, at.head_far))
    value = summed[4 * at.y_hi + at.x, 0]
    for d in range(3):
        value = value + o2_in[d, at.y_hi].astype(F32)
    y_sum.wait_recv()
    out[...] = (value + o3_in[...].astype(F32)).astype(BF16)

    for copy in started:
        copy.wait_send()
    for gather in (q, k, o):
        gather.finish_sends()
    for group in range(G):
        @pl.when(4 * group + at.g != h)
        def _(group=group):
            spread_copy(group).wait_send()


def shards(
    tokens,
    raw_keys,
    raw_values,
    query_weight,
    output_weight,
    key_expand,
    key_mix,
    key_reduce,
    value_expand,
    value_mix,
    value_reduce,
):
    kv4 = compress(
        raw_keys, raw_values, key_expand, key_mix, key_reduce, value_expand, value_mix, value_reduce
    )
    vmem = pltpu.VMEM
    dma = pltpu.SemaphoreType.DMA
    ring = [dma((4,)), dma((4,)), dma((2, 2, 4)), dma((2, 2, 4))]
    out = pl.pallas_call(
        kernel,
        out_shape=jax.ShapeDtypeStruct((160, 128), BF16),
        in_specs=[pl.BlockSpec(memory_space=vmem)] * 4,
        out_specs=pl.BlockSpec(memory_space=vmem),
        scratch_shapes=[
            vmem((4, 640, 384), BF16),
            vmem((4, 640, 512), BF16),
            vmem((2, 4, 512, KV_WIDTH), BF16),
            vmem((128, 2560), BF16),
            vmem((2, 2, 128, 384), BF16),
            vmem((128, 384), BF16),
            vmem((512, 256), BF16),
            vmem((8, 512, 512), F32),
            vmem((512, 128), F32),
            vmem((4, 128, 128), F32),
            vmem((4, 128, 128), F32),
            vmem((4, 128, 128), F32),
            vmem((4, 128, 128), BF16),
            vmem((4, 8, 128), F32),
            vmem((4, 128, 128), BF16),
            vmem((4, 8, 128), F32),
            vmem((128, 512), BF16),
            vmem((8, 2, 160, 128), F32),
            vmem((8, 2, 160, 128), BF16),
            vmem((8, 160, 128), BF16),
            vmem((2, 4, 160, 128), BF16),
            vmem((3, 2, 160, 128), BF16),
            vmem((160, 128), BF16),
            vmem((160, 128), BF16),
            *ring,
            *ring,
            *ring,
            dma((4,)),
            dma((4,)),
            dma((2, 8)),
            dma((2, 8)),
            dma((11,)),
            dma((11,)),
        ],
        compiler_params=pltpu.CompilerParams(
            collective_id=0, has_side_effects=True, vmem_limit_bytes=56 * 1024 * 1024
        ),
        name="branch",
    )(tokens, kv4, query_weight, output_weight.T)
    return out.T


def solution(mesh):
    in_specs = (
        P("seq", None),
        P(SEQ_HEAD, None),
        P(SEQ_HEAD, None),
        P("seq", "head"),
        P("head", "seq"),
        P(),
        P(),
        P(),
        P(),
        P(),
        P(),
    )
    return jax.shard_map(
        shards, mesh=mesh, in_specs=in_specs, out_specs=P("seq", "head"), check_vma=False
    )
```

```python
import jax
import jax.numpy as jnp
from jax import lax
from jax.experimental import pallas as pl
from jax.experimental.pallas import tpu as pltpu
from jax.sharding import PartitionSpec as P

G = 4
BLK = 32
STRIDE = 16
CTX = 126976
DK = 192
DV = 128
KV_WIDTH = 384
SEQ_HEAD = ("seq", "head")
MESH = pl.DeviceIdType.MESH
BF16 = jnp.bfloat16
F32 = jnp.float32
EXP2_SCALE = DK**-0.5 * 1.4426950408889634


def compress_part(raw, edge, has_next, expands, starts, mix, reduce_weight, order, moved, projected, hidden):
    moved[0:256, :] = jnp.dot(order, raw[...], preferred_element_type=F32).astype(BF16)
    moved[256:272, :] = jnp.where(has_next, edge[...], jnp.zeros_like(edge))
    row = lax.broadcasted_iota(jnp.int32, (16, 768), 0)
    for group in range(G):
        expand = expands[group]
        start = starts[group]
        projected[...] = jnp.dot(
            moved[:, start : start + expand.shape[0]], expand, preferred_element_type=F32
        )
        first = jnp.zeros((16, 768), F32)
        second = jnp.zeros((16, 768), F32)
        for p in range(STRIDE):
            block = projected[16 * p : 16 * p + 16, :]
            first = first + block * mix[p : p + 1, :]
            second = second + block * mix[STRIDE + p : STRIDE + p + 1, :]
        beyond = jnp.sum(projected[256:272, :] * mix[STRIDE:, :], axis=0, keepdims=True)
        later = jnp.where(row == 15, beyond, pltpu.roll(second, 15, 0))
        hidden[16 * group : 16 * group + 16, :] = first + later
    value = hidden[...]
    activated = (0.5 * value * (1.0 + lax.erf(value * 0.5**0.5))).astype(BF16)
    return jnp.dot(activated, reduce_weight[...], preferred_element_type=F32).astype(BF16)


class Place:
    def __init__(self):
        self.s = s = lax.axis_index("seq")
        self.h = h = lax.axis_index("head")
        self.y, self.z = s // 8, s % 8
        self.g, self.j = h // 4, h % 4
        self.core = h % 2
        self.x = (h // 2) % 4
        self.y_hi = h // 8
        self.parity = self.y % 2
        self.seq_pair = (self.y + 1 - 2 * self.parity) * 8 + self.z
        self.mate = h + 1 - 2 * self.core
        self.head_pair = h + 2 - 4 * ((h // 2) % 2)
        self.head_far = (h + 8) % 16
        self.right = self.y * 8 + (self.z + 1) % 8
        self.left = self.y * 8 + (self.z + 7) % 8

    def seq_at(self, y):
        return y * 8 + self.z


def remote(src, dst, send_sem, recv_sem, seq, head):
    return pltpu.make_async_remote_copy(
        src_ref=src,
        dst_ref=dst,
        send_sem=send_sem,
        recv_sem=recv_sem,
        device_id=(seq, head),
        device_id_type=MESH,
    )


class Gather:
    def __init__(self, at, buf, rows, sems):
        self.at, self.buf, self.rows = at, buf, rows
        self.ys, self.yr, self.zs, self.zr = sems
        self.started = []

    def piece(self, i, z):
        start = pl.multiple_of(self.rows * z, 16)
        return self.buf.at[i, pl.ds(start, self.rows), :]

    def pair(self, stream, z):
        start = pl.multiple_of(self.rows * z, 16)
        return self.buf.at[pl.ds(2 * stream, 2), pl.ds(start, self.rows), :]

    def y_copy(self, i, source):
        at = self.at
        target = (at.y + 4 - i) % 4
        return remote(
            source(target), self.piece(i, at.z), self.ys.at[i], self.yr.at[i], at.seq_at(target), at.h
        )

    def start_y(self, source):
        for i in (1, 2, 3):
            copy = self.y_copy(i, source)
            copy.start()
            self.started.append(copy)

    def wait_y(self, i, source):
        self.y_copy(i, source).wait_recv()

    def z_copy(self, way, stream, step, z):
        at = self.at
        block = self.pair(stream, z)
        return remote(
            block,
            block,
            self.zs.at[way, stream, step - 1],
            self.zr.at[way, stream, step - 1],
            (at.right, at.left)[way],
            at.h,
        )

    def ways(self, stream, step):
        return (0, 1) if step < 4 else (stream,)

    def send_z(self, stream, step):
        at = self.at
        for way in self.ways(stream, step):
            z = (at.z + 8 - (step - 1)) % 8 if way == 0 else (at.z + step - 1) % 8
            copy = self.z_copy(way, stream, step, z)
            copy.start()
            self.started.append(copy)

    def came_from(self, way, step):
        at = self.at
        return (at.z + 8 - step) % 8 if way == 0 else (at.z + step) % 8

    def wait_z(self, stream, step):
        for way in self.ways(stream, step):
            self.z_copy(way, stream, step, self.came_from(way, step)).wait_recv()

    def finish_sends(self):
        for copy in self.started:
            copy.wait_send()


def attend_half(who, at, qbuf, stacked, kvb, scores, lane_max, store):
    for half in range(2):
        for head in range(2):
            rows = pl.ds((2 * half + head) * 128, 128)
            stacked[rows, 0:DK] = qbuf[who, half, :, head * DK : (head + 1) * DK]
    last = (3 + 4 - at.y) % 4
    first_position = CTX + at.s * 128
    half_index = (at.h // 2) % 2

    def entry(n):
        return n // 4, (last + n % 4) % 4

    def score_chunk(n, masked):
        quarter, i = entry(n)
        block = lax.dot_general(
            stacked[...], kvb[quarter, i, :, 0:256], (((1,), (1,)), ((), ())), preferred_element_type=F32
        )
        parts = [block[:, 128 * k : 128 * (k + 1)] for k in range(4)]
        if masked:
            column = lax.broadcasted_iota(jnp.int32, (512, 128), 1)
            row = lax.broadcasted_iota(jnp.int32, (512, 128), 0) % 128
            ids = 256 * (30 + column // 64) + 64 * (2 * half_index + quarter) + column % 64
            visible = STRIDE * ids + BLK - 1 <= first_position + row
            parts[3] = jnp.where(visible, parts[3], -jnp.inf)
        for k in range(4):
            scores[n, :, 128 * k : 128 * (k + 1)] = parts[k]
        return jnp.maximum(jnp.maximum(parts[0], parts[1]), jnp.maximum(parts[2], parts[3]))

    lane_max[...] = jnp.maximum(score_chunk(0, True), score_chunk(4, True))

    def other_chunk(n, carry):
        lane_max[...] = jnp.maximum(lane_max[...], score_chunk(n + n // 3 + 1, False))
        return carry

    lax.fori_loop(0, 6, other_chunk, 0, unroll=6)

    for head in range(4):
        rows = slice(head * 128, (head + 1) * 128)
        row_max = jnp.max(lane_max[rows, :], axis=1, keepdims=True)

        def weigh_chunk(n, carry):
            total, numerator = carry
            exponent = jnp.exp2((scores[n, rows, :] - row_max) * EXP2_SCALE)
            for k in range(4):
                total = total + exponent[:, 128 * k : 128 * (k + 1)]
            quarter, i = entry(n)
            numerator = numerator + jnp.dot(
                exponent.astype(BF16), kvb[quarter, i, :, 256:384], preferred_element_type=F32
            )
            return total, numerator

        start = jnp.zeros((128, 128), F32)
        total, numerator = lax.fori_loop(0, 8, weigh_chunk, (start, start), unroll=8)
        store(head, row_max, jnp.sum(total, axis=1, keepdims=True), numerator)


def kernel(
    tokens,
    raw_keys,
    raw_values,
    qw,
    ow_in,
    key_expand,
    key_mix,
    key_reduce,
    value_expand,
    value_mix,
    value_reduce,
    out,
    edge_keys,
    edge_values,
    moved_keys,
    moved_values,
    placed_expand,
    projected,
    hidden,
    kv4,
    ow,
    qwb,
    owb,
    kvb,
    tokp,
    qbuf,
    qother,
    stacked,
    scores,
    lane_max,
    mine,
    mine_max,
    mine_total,
    part,
    stats,
    part_in,
    stats_in,
    attended,
    summed,
    o1,
    o1_in,
    o2,
    o2_in,
    o3,
    o3_in,
    q_ys, q_yr, q_zs, q_zr,
    k_ys, k_yr, k_zs, k_zr,
    o_ys, o_yr, o_zs, o_zr,
    r_s, r_r,
    m_s, m_r,
    e_s, e_r,
):
    at = Place()
    s, h, c = at.s, at.h, at.core

    barrier = pltpu.get_barrier_semaphore()
    partners = [(s, (h + d) % 16) for d in range(1, 16)]
    partners += [(at.seq_at((at.y + d) % 4), h) for d in (1, 2, 3)]
    partners += [(at.right, h), (at.left, h), (at.seq_pair, at.head_pair)]
    flat = 16 * s + h
    before, after = (flat + 511) % 512, (flat + 1) % 512
    partners += [(before // 16, before % 16), (after // 16, after % 16)]
    for partner in partners:
        pl.semaphore_signal(barrier, inc=1, device_id=partner, device_id_type=MESH)
    pl.semaphore_wait(barrier, len(partners))

    started = []

    def go(copy):
        copy.start()
        started.append(copy)
        return copy

    q = Gather(at, qwb, 80, (q_ys, q_yr, q_zs, q_zr))
    o = Gather(at, owb, 80, (o_ys, o_yr, o_zs, o_zr))
    k = Gather(at, kvb.at[c], 64, (k_ys, k_yr, k_zs, k_zr))

    edge_in = [
        remote(source.at[0:16], target, e_s.at[i], e_r.at[i], before // 16, before % 16)
        for i, (source, target) in enumerate(((raw_keys, edge_keys), (raw_values, edge_values)), 11)
    ]
    for copy in edge_in:
        go(copy)

    def q_source(target):
        return qw.at[:, pl.ds(pl.multiple_of(384 * (target % 2), 128), 384)]

    q.start_y(q_source)
    half_tokens = pl.ds(pl.multiple_of(1280 * c, 128), 1280)
    tok_copy = go(
        remote(
            tokens.at[:, half_tokens], tokp.at[:, half_tokens], e_s.at[0], e_r.at[0], at.seq_pair, h
        )
    )
    qwb[0, pl.ds(pl.multiple_of(80 * at.z, 16), 80), :] = qw[
        :, pl.ds(pl.multiple_of(384 * at.parity, 128), 384)
    ]

    same = lax.broadcasted_iota(jnp.int32, (80, 80), 0) == lax.broadcasted_iota(jnp.int32, (80, 80), 1)
    ow[...] = lax.dot_general(
        same.astype(F32).astype(BF16), ow_in[...], (((1,), (1,)), ((), ())), preferred_element_type=F32
    ).astype(BF16)
    owb[0, pl.ds(pl.multiple_of(80 * at.z, 16), 80), :] = ow[...]
    placed_expand[0, 0:DK, :] = key_expand[...]
    placed_expand[0, DK:256, :] = jnp.zeros((256 - DK, 768), BF16)
    placed_expand[1, 0 : 256 - DK, :] = jnp.zeros((256 - DK, 768), BF16)
    placed_expand[1, 256 - DK :, :] = key_expand[...]
    stacked[:, DK:] = jnp.zeros((512, 256 - DK), BF16)

    q.wait_y(1, q_source)
    q.send_z(0, 1)
    q.wait_y(2, q_source)
    q.wait_y(3, q_source)
    q.send_z(1, 1)

    row = lax.broadcasted_iota(jnp.int32, (256, 256), 0)
    column = lax.broadcasted_iota(jnp.int32, (256, 256), 1)
    order = (column == 16 * (row % 16) + row // 16).astype(F32).astype(BF16)
    for copy in edge_in:
        copy.wait_recv()
    has_next = flat < 511
    packed_keys = compress_part(
        raw_keys,
        edge_keys,
        has_next,
        [placed_expand[group % 2] for group in range(G)],
        (0, 128, 384, 512),
        key_mix,
        key_reduce,
        order,
        moved_keys,
        projected,
        hidden,
    )
    packed_values = compress_part(
        raw_values,
        edge_values,
        has_next,
        [value_expand[...]] * G,
        (0, 128, 256, 384),
        value_mix,
        value_reduce,
        order,
        moved_values,
        projected,
        hidden,
    )
    for group in range(G):
        rows = slice(16 * group, 16 * group + 16)
        kv4[group, :, 0:DK] = packed_keys[rows, :]
        kv4[group, :, DK:256] = jnp.zeros((16, 256 - DK), BF16)
        kv4[group, :, 256:384] = packed_values[rows, :]

    own_rows = pl.ds(pl.multiple_of(64 * at.z + 16 * at.j, 16), 16)

    def spread_copy(group):
        quarter = at.g % 2
        return remote(
            kv4.at[group],
            kvb.at[quarter, 0, own_rows, :],
            r_s.at[group],
            r_r.at[at.j],
            s,
            4 * group + at.g,
        )

    for group in range(G):
        @pl.when(4 * group + at.g != h)
        def _(group=group):
            spread_copy(group).start()

        @pl.when(4 * group + at.g == h)
        def _(group=group):
            kvb[c, 0, own_rows, :] = kv4[group]

    def k_source(target):
        return k.piece(0, at.z)

    def ow_source(target):
        return ow

    def mate_copy(quarter, stream, index, z):
        start = pl.multiple_of(64 * z, 16)
        block = kvb.at[quarter, pl.ds(2 * stream, 2), pl.ds(start, 64), :]
        return remote(
            block, block, m_s.at[stream, index], m_r.at[stream, index], s, at.mate
        )

    def k_arrived(stream, step):
        k.wait_z(stream, step)
        for way in k.ways(stream, step):
            index = 7 if step == 4 else 3 * way + step
            go(mate_copy(c, stream, index, k.came_from(way, step)))

    def q_round(step):
        for stream in (0, 1):
            q.wait_z(stream, step - 1)
            q.send_z(stream, step)

    def k_round(step):
        for stream in (0, 1):
            k_arrived(stream, step - 1)
            k.send_z(stream, step)

    q_round(2)
    for m in range(4):
        @pl.when(4 * at.j + m != h)
        def _(m=m):
            rows = pl.ds(pl.multiple_of(64 * at.z + 16 * m, 16), 16)
            remote(
                kv4.at[0], kvb.at[c, 0, rows, :], r_s.at[0], r_r.at[m], s, 4 * at.j + m
            ).wait_recv()
    k.start_y(k_source)
    o.start_y(ow_source)
    q_round(3)
    k.wait_y(1, k_source)
    k.send_z(0, 1)
    go(mate_copy(c, 0, 0, at.z))
    k.wait_y(2, k_source)
    k.wait_y(3, k_source)
    k.send_z(1, 1)
    go(mate_copy(c, 1, 0, at.z))
    tok_copy.wait_recv()
    arrived_tokens = tokp.at[:, half_tokens]
    go(remote(arrived_tokens, arrived_tokens, e_s.at[13], e_r.at[13], s, at.mate))
    q_round(4)
    k_round(2)
    other_half = tokp.at[:, pl.ds(pl.multiple_of(1280 - 1280 * c, 128), 1280)]
    remote(other_half, other_half, e_s.at[13], e_r.at[13], s, at.mate).wait_recv()
    q.wait_z(0, 4)
    q.wait_z(1, 4)

    def project_queries(source):
        total = jnp.zeros((128, 384), F32)
        for i in range(4):
            start = pl.multiple_of(640 * ((at.y + i) % 4), 128)
            total = total + jnp.dot(
                source[:, pl.ds(start, 640)], qwb[i], preferred_element_type=F32
            )
        return total.astype(BF16)

    qother[...] = project_queries(tokp)
    q_in = [
        remote(qother, qbuf.at[0, at.parity], e_s.at[1], e_r.at[1], at.seq_pair, h),
        remote(qother, qbuf.at[1, at.parity], e_s.at[2], e_r.at[2], at.seq_pair, at.head_pair),
    ]
    go(q_in[0])
    go(q_in[1])
    qbuf[0, at.parity] = project_queries(tokens)
    q_in.append(
        go(
            remote(
                qbuf.at[0, at.parity], qbuf.at[1, at.parity], e_s.at[3], e_r.at[3], s, at.head_pair
            )
        )
    )
    k_round(3)
    k_round(4)
    o.wait_y(1, ow_source)
    o.send_z(0, 1)
    o.wait_y(2, ow_source)
    o.wait_y(3, ow_source)
    o.send_z(1, 1)
    k_arrived(0, 4)
    k_arrived(1, 4)
    q_in[0].wait_recv()
    q_in[2].wait_recv()
    q_in[1].wait_recv()
    for stream in (0, 1):
        mate_copy(1 - c, stream, 0, at.z).wait_recv()
        for step in (1, 2, 3, 4):
            for way in k.ways(stream, step):
                index = 7 if step == 4 else 3 * way + step
                mate_copy(1 - c, stream, index, k.came_from(way, step)).wait_recv()

    lane = lax.broadcasted_iota(jnp.int32, (128, 128), 1)

    def store_part(head, row_max, row_total, numerator):
        part[head] = numerator.astype(BF16)
        tile = jnp.where(lane == 0, row_max, jnp.where(lane == 1, row_total, 0.0))
        stats[head] = jnp.transpose(tile)[0:8, :]

    attend_half(1, at, qbuf, stacked, kvb, scores, lane_max, store_part)
    part_copy = go(remote(part, part_in, e_s.at[4], e_r.at[4], s, at.head_pair))
    stat_copy = go(remote(stats, stats_in, e_s.at[5], e_r.at[5], s, at.head_pair))
    for stream in (0, 1):
        o.wait_z(stream, 1)
        o.send_z(stream, 2)

    def store_mine(head, row_max, row_total, numerator):
        mine[head] = numerator
        mine_max[head] = jnp.broadcast_to(row_max, (128, 128))
        mine_total[head] = jnp.broadcast_to(row_total, (128, 128))

    attend_half(0, at, qbuf, stacked, kvb, scores, lane_max, store_mine)
    for stream in (0, 1):
        o.wait_z(stream, 2)
        o.send_z(stream, 3)
    part_copy.wait_recv()
    stat_copy.wait_recv()
    for head in range(4):
        tile = jnp.concatenate([stats_in[head], jnp.zeros((120, 128), F32)], axis=0)
        tile = jnp.transpose(tile)
        other_max = jnp.broadcast_to(tile[:, 0:1], (128, 128))
        other_total = jnp.broadcast_to(tile[:, 1:2], (128, 128))
        top = jnp.maximum(mine_max[head], other_max)
        own_part = jnp.exp2((mine_max[head] - top) * EXP2_SCALE)
        other_part = jnp.exp2((other_max - top) * EXP2_SCALE)
        total = mine_total[head] * own_part + other_total * other_part
        value = mine[head] * own_part + part_in[head].astype(F32) * other_part
        attended[:, head * DV : (head + 1) * DV] = (value / total).astype(BF16)
    for stream in (0, 1):
        o.wait_z(stream, 3)
        o.send_z(stream, 4)
    o.wait_z(0, 4)
    o.wait_z(1, 4)

    for i in range(4):
        start = pl.multiple_of(4 * ((at.y + i) % 4), 4)
        block = lax.dot_general(
            owb[i], attended[...], (((1,), (1,)), ((), ())), preferred_element_type=F32
        ).reshape(2, 2, 160, 128)
        summed[pl.ds(2 * ((at.y + i) % 4), 2)] = block
        o1[pl.ds(2 * ((at.y + i) % 4), 2)] = block.astype(BF16)
    mate_sum = go(remote(o1.at[:, 1 - c], o1_in, e_s.at[6], e_r.at[6], s, at.mate))
    mate_sum.wait_recv()
    for i in range(8):
        summed[i, 0] = summed[i, c] + o1_in[i].astype(F32)
        o2[i // 4, i % 4] = summed[i, 0].astype(BF16)
    x_sums = []
    for d in (1, 2, 3):
        x = (at.x + d) % 4
        x_sums.append(
            go(
                remote(
                    o2.at[:, x], o2_in.at[d - 1], e_s.at[6 + d], e_r.at[6 + d], s, 8 * at.y_hi + 2 * x + c
                )
            )
        )
    for copy in x_sums:
        copy.wait_recv()
    far = 1 - at.y_hi
    value = summed[4 * far + at.x, 0]
    for d in range(3):
        value = value + o2_in[d, far].astype(F32)
    o3[...] = value.astype(BF16)
    y_sum = go(remote(o3, o3_in, e_s.at[10], e_r.at[10], s, at.head_far))
    value = summed[4 * at.y_hi + at.x, 0]
    for d in range(3):
        value = value + o2_in[d, at.y_hi].astype(F32)
    y_sum.wait_recv()
    out[...] = (value + o3_in[...].astype(F32)).astype(BF16)

    for copy in started:
        copy.wait_send()
    for gather in (q, k, o):
        gather.finish_sends()
    for group in range(G):
        @pl.when(4 * group + at.g != h)
        def _(group=group):
            spread_copy(group).wait_send()


def shards(
    tokens,
    raw_keys,
    raw_values,
    query_weight,
    output_weight,
    key_expand,
    key_mix,
    key_reduce,
    value_expand,
    value_mix,
    value_reduce,
):
    vmem = pltpu.VMEM
    dma = pltpu.SemaphoreType.DMA
    ring = [dma((4,)), dma((4,)), dma((2, 2, 4)), dma((2, 2, 4))]
    out = pl.pallas_call(
        kernel,
        out_shape=jax.ShapeDtypeStruct((160, 128), BF16),
        in_specs=[pl.BlockSpec(memory_space=vmem)] * 11,
        out_specs=pl.BlockSpec(memory_space=vmem),
        scratch_shapes=[
            vmem((16, 768), BF16),
            vmem((16, 512), BF16),
            vmem((272, 768), BF16),
            vmem((272, 512), BF16),
            vmem((2, 256, 768), BF16),
            vmem((272, 768), F32),
            vmem((64, 768), F32),
            vmem((G, 16, KV_WIDTH), BF16),
            vmem((80, 512), BF16),
            vmem((4, 640, 384), BF16),
            vmem((4, 640, 512), BF16),
            vmem((2, 4, 512, KV_WIDTH), BF16),
            vmem((128, 2560), BF16),
            vmem((2, 2, 128, 384), BF16),
            vmem((128, 384), BF16),
            vmem((512, 256), BF16),
            vmem((8, 512, 512), F32),
            vmem((512, 128), F32),
            vmem((4, 128, 128), F32),
            vmem((4, 128, 128), F32),
            vmem((4, 128, 128), F32),
            vmem((4, 128, 128), BF16),
            vmem((4, 8, 128), F32),
            vmem((4, 128, 128), BF16),
            vmem((4, 8, 128), F32),
            vmem((128, 512), BF16),
            vmem((8, 2, 160, 128), F32),
            vmem((8, 2, 160, 128), BF16),
            vmem((8, 160, 128), BF16),
            vmem((2, 4, 160, 128), BF16),
            vmem((3, 2, 160, 128), BF16),
            vmem((160, 128), BF16),
            vmem((160, 128), BF16),
            *ring,
            *ring,
            *ring,
            dma((4,)),
            dma((4,)),
            dma((2, 8)),
            dma((2, 8)),
            dma((14,)),
            dma((14,)),
        ],
        compiler_params=pltpu.CompilerParams(
            collective_id=0, has_side_effects=True, vmem_limit_bytes=56 * 1024 * 1024
        ),
        name="branch",
    )(
        tokens,
        raw_keys,
        raw_values,
        query_weight,
        output_weight,
        key_expand,
        key_mix,
        key_reduce,
        value_expand,
        value_mix,
        value_reduce,
    )
    return out.T


def solution(mesh):
    in_specs = (
        P("seq", None),
        P(SEQ_HEAD, None),
        P(SEQ_HEAD, None),
        P("seq", "head"),
        P("head", "seq"),
        P(),
        P(),
        P(),
        P(),
        P(),
        P(),
    )
    return jax.shard_map(
        shards, mesh=mesh, in_specs=in_specs, out_specs=P("seq", "head"), check_vma=False
    )
```

```python
import jax
import jax.numpy as jnp
from jax import lax
from jax.experimental import pallas as pl
from jax.experimental.pallas import tpu as pltpu
from jax.sharding import PartitionSpec as P

G = 4
BLK = 32
STRIDE = 16
CTX = 126976
DK = 192
DV = 128
KV_WIDTH = 384
SEQ_HEAD = ("seq", "head")
MESH = pl.DeviceIdType.MESH
BF16 = jnp.bfloat16
F32 = jnp.float32
EXP2_SCALE = DK**-0.5 * 1.4426950408889634


def compress_part(
    raw, edge, has_next, expands, starts, mix, reduce_weight, reduce_dim, order, moved, projected, hidden
):
    moved[0:256, :] = jnp.dot(order, raw[...], preferred_element_type=F32).astype(BF16)
    moved[256:272, :] = jnp.where(has_next, edge[...], jnp.zeros_like(edge))
    row = lax.broadcasted_iota(jnp.int32, (16, 768), 0)
    for group in range(G):
        expand = expands[group]
        start = starts[group]
        projected[...] = jnp.dot(
            moved[:, start : start + expand.shape[0]], expand, preferred_element_type=F32
        )
        first = jnp.zeros((16, 768), F32)
        second = jnp.zeros((16, 768), F32)
        for p in range(STRIDE):
            block = projected[16 * p : 16 * p + 16, :]
            first = first + block * mix[p : p + 1, :]
            second = second + block * mix[STRIDE + p : STRIDE + p + 1, :]
        beyond = jnp.sum(projected[256:272, :] * mix[STRIDE:, :], axis=0, keepdims=True)
        later = jnp.where(row == 15, beyond, pltpu.roll(second, 15, 0))
        hidden[16 * group : 16 * group + 16, :] = first + later
    value = hidden[...]
    activated = (0.5 * value * (1.0 + lax.erf(value * 0.5**0.5))).astype(BF16)
    return lax.dot_general(
        activated, reduce_weight[...], (((1,), (reduce_dim,)), ((), ())), preferred_element_type=F32
    ).astype(BF16)


class Place:
    def __init__(self):
        self.s = s = lax.axis_index("seq")
        self.h = h = lax.axis_index("head")
        self.y, self.z = s // 8, s % 8
        self.g, self.j = h // 4, h % 4
        self.core = h % 2
        self.x = (h // 2) % 4
        self.y_hi = h // 8
        self.parity = self.y % 2
        self.seq_pair = (self.y + 1 - 2 * self.parity) * 8 + self.z
        self.mate = h + 1 - 2 * self.core
        self.head_pair = h + 2 - 4 * ((h // 2) % 2)
        self.head_far = (h + 8) % 16
        self.right = self.y * 8 + (self.z + 1) % 8
        self.left = self.y * 8 + (self.z + 7) % 8

    def seq_at(self, y):
        return y * 8 + self.z


def remote(src, dst, send_sem, recv_sem, seq, head):
    return pltpu.make_async_remote_copy(
        src_ref=src,
        dst_ref=dst,
        send_sem=send_sem,
        recv_sem=recv_sem,
        device_id=(seq, head),
        device_id_type=MESH,
    )


class Gather:
    def __init__(self, at, buf, rows, streams, sems):
        self.at, self.buf, self.rows, self.streams = at, buf, rows, streams
        self.ys, self.yr, self.zs, self.zr = sems
        self.started = []

    def piece(self, i, z):
        start = pl.multiple_of(self.rows * z, 16)
        return self.buf.at[i, pl.ds(start, self.rows), :]

    def block(self, stream, z):
        first, count, _ = self.streams[stream]
        start = pl.multiple_of(self.rows * z, 16)
        return self.buf.at[pl.ds(first, count), pl.ds(start, self.rows), :]

    def y_copy(self, i, source):
        at = self.at
        target = (at.y + 4 - i) % 4
        return remote(
            source(target), self.piece(i, at.z), self.ys.at[i], self.yr.at[i], at.seq_at(target), at.h
        )

    def start_y(self, source):
        for i in (1, 2, 3):
            copy = self.y_copy(i, source)
            copy.start()
            self.started.append(copy)

    def first_z(self, source, streams):
        for stream in streams:
            first, count, _ = self.streams[stream]
            for i in range(first, first + count):
                if i > 0:
                    self.y_copy(i, source).wait_recv()
            self.send_z(stream, 1)

    def z_copy(self, way, stream, step, z):
        at = self.at
        block = self.block(stream, z)
        return remote(
            block,
            block,
            self.zs.at[way, stream, step - 1],
            self.zr.at[way, stream, step - 1],
            (at.right, at.left)[way],
            at.h,
        )

    def ways(self, stream, step):
        return (0, 1) if step < 4 else (self.streams[stream][2],)

    def send_z(self, stream, step):
        at = self.at
        for way in self.ways(stream, step):
            z = (at.z + 8 - (step - 1)) % 8 if way == 0 else (at.z + step - 1) % 8
            copy = self.z_copy(way, stream, step, z)
            copy.start()
            self.started.append(copy)

    def came_from(self, way, step):
        at = self.at
        return (at.z + 8 - step) % 8 if way == 0 else (at.z + step) % 8

    def wait_z(self, stream, step):
        for way in self.ways(stream, step):
            self.z_copy(way, stream, step, self.came_from(way, step)).wait_recv()

    def next_z(self, step):
        for stream in range(len(self.streams)):
            self.wait_z(stream, step - 1)
            self.send_z(stream, step)

    def end_z(self):
        for stream in range(len(self.streams)):
            self.wait_z(stream, 4)

    def finish_sends(self):
        for copy in self.started:
            copy.wait_send()


class HalfGather(Gather):
    def half_copy(self, n, source):
        at = self.at
        i = at.y % 2
        target = at.y // 2 + 2 * n
        return target, remote(
            source, self.piece(i, at.z), self.ys.at[n], self.yr.at[i], at.seq_at(target), at.h
        )

    def start_half(self, source):
        at = self.at
        for n in range(2):
            target, copy = self.half_copy(n, source)

            @pl.when(target != at.y)
            def _(copy=copy):
                copy.start()

            @pl.when(target == at.y)
            def _():
                start = pl.multiple_of(self.rows * at.z, 16)
                self.buf[at.y % 2, pl.ds(start, self.rows), :] = source[...]

    def wait_half(self, i, source):
        at = self.at
        origin = 2 * at.parity + i

        @pl.when(origin != at.y)
        def _():
            remote(
                source, self.piece(i, at.z), self.ys.at[i], self.yr.at[i], at.seq_at(origin), at.h
            ).wait_recv()

    def end_half(self, source):
        for n in range(2):
            target, copy = self.half_copy(n, source)

            @pl.when(target != self.at.y)
            def _(copy=copy):
                copy.wait_send()


QUARTERS = ((0, 1, 0), (1, 2, 1), (3, 1, 0))
HALVES = ((0, 1, 0), (1, 1, 1))


def attend_half(who, at, qbuf, stacked, kvb, scores, lane_max, store):
    for half in range(2):
        for head in range(2):
            rows = pl.ds((2 * half + head) * 128, 128)
            stacked[rows, 0:DK] = qbuf[who, half, :, head * DK : (head + 1) * DK]
    last = (3 + 4 - at.y) % 4
    first_position = CTX + at.s * 128
    half_index = (at.h // 2) % 2

    def entry(n):
        return n // 4, (last + n % 4) % 4

    def score_chunk(n, masked):
        quarter, i = entry(n)
        block = lax.dot_general(
            stacked[...], kvb[quarter, i, :, 0:256], (((1,), (1,)), ((), ())), preferred_element_type=F32
        )
        parts = [block[:, 128 * k : 128 * (k + 1)] for k in range(4)]
        if masked:
            column = lax.broadcasted_iota(jnp.int32, (512, 128), 1)
            row = lax.broadcasted_iota(jnp.int32, (512, 128), 0) % 128
            ids = 256 * (30 + column // 64) + 64 * (2 * half_index + quarter) + column % 64
            visible = STRIDE * ids + BLK - 1 <= first_position + row
            parts[3] = jnp.where(visible, parts[3], -jnp.inf)
        for k in range(4):
            scores[n, :, 128 * k : 128 * (k + 1)] = parts[k]
        return jnp.maximum(jnp.maximum(parts[0], parts[1]), jnp.maximum(parts[2], parts[3]))

    lane_max[...] = jnp.maximum(score_chunk(0, True), score_chunk(4, True))

    def other_chunk(n, carry):
        lane_max[...] = jnp.maximum(lane_max[...], score_chunk(n + n // 3 + 1, False))
        return carry

    lax.fori_loop(0, 6, other_chunk, 0, unroll=6)

    for head in range(4):
        rows = slice(head * 128, (head + 1) * 128)
        row_max = jnp.max(lane_max[rows, :], axis=1, keepdims=True)

        def weigh_chunk(n, carry):
            total, numerator = carry
            exponent = jnp.exp2((scores[n, rows, :] - row_max) * EXP2_SCALE)
            for k in range(4):
                total = total + exponent[:, 128 * k : 128 * (k + 1)]
            quarter, i = entry(n)
            numerator = numerator + jnp.dot(
                exponent.astype(BF16), kvb[quarter, i, :, 256:384], preferred_element_type=F32
            )
            return total, numerator

        start = jnp.zeros((128, 128), F32)
        total, numerator = lax.fori_loop(0, 8, weigh_chunk, (start, start), unroll=8)
        store(head, row_max, jnp.sum(total, axis=1, keepdims=True), numerator)


def kernel(
    tokens,
    raw_keys,
    raw_values,
    qw,
    ow,
    key_expand,
    key_mix,
    key_reduce,
    value_expand,
    value_mix,
    value_reduce,
    out,
    edge_keys,
    edge_values,
    moved_keys,
    moved_values,
    placed_expand,
    projected,
    hidden,
    kv4,
    qwb,
    owb,
    kvb,
    tokp,
    qbuf,
    qother,
    stacked,
    scores,
    lane_max,
    mine,
    mine_max,
    mine_total,
    part,
    stats,
    part_in,
    stats_in,
    attended,
    summed,
    o1,
    o1_in,
    o2,
    o2_in,
    o3,
    o3_in,
    q_ys, q_yr, q_zs, q_zr,
    k_ys, k_yr, k_zs, k_zr,
    o_ys, o_yr, o_zs, o_zr,
    r_s, r_r,
    m_s, m_r,
    e_s, e_r,
):
    at = Place()
    s, h, c = at.s, at.h, at.core

    barrier = pltpu.get_barrier_semaphore()
    partners = [(s, (h + d) % 16) for d in range(1, 16)]
    partners += [(at.seq_at((at.y + d) % 4), h) for d in (1, 2, 3)]
    partners += [(at.right, h), (at.left, h)]
    partners += [(at.seq_pair, at.head_pair), (at.seq_pair, at.head_far)]
    flat = 16 * s + h
    before, after = (flat + 511) % 512, (flat + 1) % 512
    partners += [(before // 16, before % 16), (after // 16, after % 16)]
    for partner in partners:
        pl.semaphore_signal(barrier, inc=1, device_id=partner, device_id_type=MESH)
    pl.semaphore_wait(barrier, len(partners))

    started = []

    def go(copy):
        copy.start()
        started.append(copy)
        return copy

    q = Gather(at, qwb, 80, QUARTERS, (q_ys, q_yr, q_zs, q_zr))
    o = HalfGather(at, owb, 80, HALVES, (o_ys, o_yr, o_zs, o_zr))
    k = Gather(at, kvb.at[c], 64, QUARTERS, (k_ys, k_yr, k_zs, k_zr))

    edge_in = [
        remote(source.at[0:16], target, e_s.at[i], e_r.at[i], before // 16, before % 16)
        for i, (source, target) in enumerate(((raw_keys, edge_keys), (raw_values, edge_values)), 11)
    ]
    for copy in edge_in:
        go(copy)

    def q_source(target):
        return qw.at[:, pl.ds(pl.multiple_of(384 * (target % 2), 128), 384)]

    qwb[0, pl.ds(pl.multiple_of(80 * at.z, 16), 80), :] = qw[
        :, pl.ds(pl.multiple_of(384 * at.parity, 128), 384)
    ]
    q.start_y(q_source)
    q.first_z(q_source, (0,))
    half_tokens = pl.ds(pl.multiple_of(1280 * c, 128), 1280)
    tok_copy = go(
        remote(
            tokens.at[:, half_tokens], tokp.at[:, half_tokens], e_s.at[0], e_r.at[0], at.seq_pair, h
        )
    )
    placed_expand[0, 0:DK, :] = key_expand[...]
    placed_expand[0, DK:256, :] = jnp.zeros((256 - DK, 768), BF16)
    placed_expand[1, 0 : 256 - DK, :] = jnp.zeros((256 - DK, 768), BF16)
    placed_expand[1, 256 - DK :, :] = key_expand[...]
    stacked[:, DK:] = jnp.zeros((512, 256 - DK), BF16)

    q.first_z(q_source, (1, 2))

    row = lax.broadcasted_iota(jnp.int32, (256, 256), 0)
    column = lax.broadcasted_iota(jnp.int32, (256, 256), 1)
    order = (column == 16 * (row % 16) + row // 16).astype(F32).astype(BF16)
    for copy in edge_in:
        copy.wait_recv()
    has_next = flat < 511
    packed_keys = compress_part(
        raw_keys,
        edge_keys,
        has_next,
        [placed_expand[group % 2] for group in range(G)],
        (0, 128, 384, 512),
        key_mix,
        key_reduce,
        1,
        order,
        moved_keys,
        projected,
        hidden,
    )
    packed_values = compress_part(
        raw_values,
        edge_values,
        has_next,
        [value_expand[...]] * G,
        (0, 128, 256, 384),
        value_mix,
        value_reduce,
        0,
        order,
        moved_values,
        projected,
        hidden,
    )
    for group in range(G):
        rows = slice(16 * group, 16 * group + 16)
        kv4[group, :, 0:DK] = packed_keys[rows, :]
        kv4[group, :, DK:256] = jnp.zeros((16, 256 - DK), BF16)
        kv4[group, :, 256:384] = packed_values[rows, :]

    own_rows = pl.ds(pl.multiple_of(64 * at.z + 16 * at.j, 16), 16)

    def spread_copy(group):
        quarter = at.g % 2
        return remote(
            kv4.at[group],
            kvb.at[quarter, 0, own_rows, :],
            r_s.at[group],
            r_r.at[at.j],
            s,
            4 * group + at.g,
        )

    for group in range(G):
        @pl.when(4 * group + at.g != h)
        def _(group=group):
            spread_copy(group).start()

        @pl.when(4 * group + at.g == h)
        def _(group=group):
            kvb[c, 0, own_rows, :] = kv4[group]

    def k_source(target):
        return k.piece(0, at.z)

    def mate_copy(quarter, stream, index, z):
        first, count, _ = QUARTERS[stream]
        start = pl.multiple_of(64 * z, 16)
        block = kvb.at[quarter, pl.ds(first, count), pl.ds(start, 64), :]
        return remote(
            block, block, m_s.at[stream, index], m_r.at[stream, index], s, at.mate
        )

    def k_arrived(stream, step):
        k.wait_z(stream, step)
        for way in k.ways(stream, step):
            index = 7 if step == 4 else 3 * way + step
            go(mate_copy(c, stream, index, k.came_from(way, step)))

    def k_round(step):
        for stream in (0, 1, 2):
            k_arrived(stream, step - 1)
            k.send_z(stream, step)

    q.next_z(2)
    for m in range(4):
        @pl.when(4 * at.j + m != h)
        def _(m=m):
            rows = pl.ds(pl.multiple_of(64 * at.z + 16 * m, 16), 16)
            remote(
                kv4.at[0], kvb.at[c, 0, rows, :], r_s.at[0], r_r.at[m], s, 4 * at.j + m
            ).wait_recv()
    k.start_y(k_source)
    o.start_half(ow)
    for stream in (0, 1, 2):
        if stream == 2:
            q.next_z(3)
        k.first_z(k_source, (stream,))
        go(mate_copy(c, stream, 0, at.z))
    tok_copy.wait_recv()
    arrived_tokens = tokp.at[:, half_tokens]
    go(remote(arrived_tokens, arrived_tokens, e_s.at[13], e_r.at[13], s, at.mate))
    q.next_z(4)
    k_round(2)
    other_half = tokp.at[:, pl.ds(pl.multiple_of(1280 - 1280 * c, 128), 1280)]
    remote(other_half, other_half, e_s.at[13], e_r.at[13], s, at.mate).wait_recv()
    q.end_z()

    def project_queries(source):
        total = jnp.zeros((128, 384), F32)
        for i in range(4):
            start = pl.multiple_of(640 * ((at.y + i) % 4), 128)
            total = total + jnp.dot(
                source[:, pl.ds(start, 640)], qwb[i], preferred_element_type=F32
            )
        return total.astype(BF16)

    qother[...] = project_queries(tokp)
    q_in = [
        remote(qother, qbuf.at[0, at.parity], e_s.at[1], e_r.at[1], at.seq_pair, h),
        remote(qother, qbuf.at[1, at.parity], e_s.at[2], e_r.at[2], at.seq_pair, at.head_pair),
    ]
    go(q_in[0])
    go(q_in[1])
    qbuf[0, at.parity] = project_queries(tokens)
    q_in.append(
        go(
            remote(
                qbuf.at[0, at.parity], qbuf.at[1, at.parity], e_s.at[3], e_r.at[3], s, at.head_pair
            )
        )
    )
    k_round(3)
    for i in (0, 1):
        o.wait_half(i, ow)
        o.send_z(i, 1)
    k_round(4)
    o.next_z(2)
    for stream in (0, 1, 2):
        k_arrived(stream, 4)
    q_in[0].wait_recv()
    q_in[2].wait_recv()
    q_in[1].wait_recv()
    for stream in (0, 1, 2):
        mate_copy(1 - c, stream, 0, at.z).wait_recv()
        for step in (1, 2, 3, 4):
            for way in k.ways(stream, step):
                index = 7 if step == 4 else 3 * way + step
                mate_copy(1 - c, stream, index, k.came_from(way, step)).wait_recv()

    lane = lax.broadcasted_iota(jnp.int32, (128, 128), 1)

    def store_part(head, row_max, row_total, numerator):
        part[head] = numerator.astype(BF16)
        tile = jnp.where(lane == 0, row_max, jnp.where(lane == 1, row_total, 0.0))
        stats[head] = jnp.transpose(tile)[0:8, :]

    attend_half(1, at, qbuf, stacked, kvb, scores, lane_max, store_part)
    part_copy = go(remote(part, part_in, e_s.at[4], e_r.at[4], s, at.head_pair))
    stat_copy = go(remote(stats, stats_in, e_s.at[5], e_r.at[5], s, at.head_pair))
    o.next_z(3)

    def store_mine(head, row_max, row_total, numerator):
        mine[head] = numerator
        mine_max[head] = jnp.broadcast_to(row_max, (128, 128))
        mine_total[head] = jnp.broadcast_to(row_total, (128, 128))

    attend_half(0, at, qbuf, stacked, kvb, scores, lane_max, store_mine)
    part_copy.wait_recv()
    stat_copy.wait_recv()
    for head in range(4):
        tile = jnp.concatenate([stats_in[head], jnp.zeros((120, 128), F32)], axis=0)
        tile = jnp.transpose(tile)
        other_max = jnp.broadcast_to(tile[:, 0:1], (128, 128))
        other_total = jnp.broadcast_to(tile[:, 1:2], (128, 128))
        top = jnp.maximum(mine_max[head], other_max)
        own_part = jnp.exp2((mine_max[head] - top) * EXP2_SCALE)
        other_part = jnp.exp2((other_max - top) * EXP2_SCALE)
        total = mine_total[head] * own_part + other_total * other_part
        value = mine[head] * own_part + part_in[head].astype(F32) * other_part
        attended[0:128, head * DV : (head + 1) * DV] = (value / total).astype(BF16)
    attended_copy = go(
        remote(
            attended.at[0:128], attended.at[128:256], e_s.at[6], e_r.at[6], at.seq_pair, h
        )
    )
    o.next_z(4)
    o.end_z()
    attended_copy.wait_recv()

    for i in range(2):
        block = lax.dot_general(
            owb[i], attended[...], (((1,), (1,)), ((), ())), preferred_element_type=F32
        ).reshape(2, 2, 160, 256)
        summed[2 * i : 2 * i + 2] = block
        o1[2 * i : 2 * i + 2] = block.astype(BF16)
    mate_sum = go(remote(o1.at[:, 1 - c], o1_in, e_s.at[14], e_r.at[14], s, at.mate))
    mate_sum.wait_recv()
    for x in range(4):
        summed[x, 0] = summed[x, c] + o1_in[x].astype(F32)
        o2[x] = summed[x, 0].astype(BF16)
    x_sums = []
    for d in (1, 2, 3):
        x = (at.x + d) % 4
        x_sums.append(
            go(
                remote(
                    o2.at[x], o2_in.at[d - 1], e_s.at[6 + d], e_r.at[6 + d], s, 8 * at.y_hi + 2 * x + c
                )
            )
        )
    for copy in x_sums:
        copy.wait_recv()
    value = summed[at.x, 0]
    for d in range(3):
        value = value + o2_in[d].astype(F32)
    own, other = value[:, 0:128], value[:, 128:256]
    o3[0] = own.astype(BF16)
    o3[1] = other.astype(BF16)
    own_sum = remote(o3.at[0], o3_in.at[1], e_s.at[10], e_r.at[10], s, at.head_far)
    pair_sum = remote(o3.at[1], o3_in.at[0], e_s.at[15], e_r.at[15], at.seq_pair, h)
    cross_sum = remote(o3.at[1], o3_in.at[1], e_s.at[10 + 6], e_r.at[10], at.seq_pair, at.head_far)

    @pl.when(at.y_hi == at.parity)
    def _():
        pair_sum.start()
        own_sum.wait_recv()
        out[...] = (own + o3_in[1].astype(F32)).astype(BF16)
        pair_sum.wait_send()

    @pl.when(at.y_hi != at.parity)
    def _():
        cross_sum.start()
        own_sum.start()
        pair_sum.wait_recv()
        cross_sum.wait_recv()
        out[...] = (o3_in[0].astype(F32) + o3_in[1].astype(F32)).astype(BF16)
        cross_sum.wait_send()
        own_sum.wait_send()

    for copy in started:
        copy.wait_send()
    for gather in (q, k, o):
        gather.finish_sends()
    o.end_half(ow)
    for group in range(G):
        @pl.when(4 * group + at.g != h)
        def _(group=group):
            spread_copy(group).wait_send()


def shards(
    tokens,
    raw_keys,
    raw_values,
    query_weight,
    output_weight,
    key_expand,
    key_mix,
    key_reduce,
    value_expand,
    value_mix,
    value_reduce,
):
    vmem = pltpu.VMEM
    dma = pltpu.SemaphoreType.DMA
    ring = [dma((4,)), dma((4,)), dma((2, 3, 4)), dma((2, 3, 4))]
    out = pl.pallas_call(
        kernel,
        out_shape=jax.ShapeDtypeStruct((160, 128), BF16),
        in_specs=[pl.BlockSpec(memory_space=vmem)] * 11,
        out_specs=pl.BlockSpec(memory_space=vmem),
        scratch_shapes=[
            vmem((16, 768), BF16),
            vmem((16, 512), BF16),
            vmem((272, 768), BF16),
            vmem((272, 512), BF16),
            vmem((2, 256, 768), BF16),
            vmem((272, 768), F32),
            vmem((64, 768), F32),
            vmem((G, 16, KV_WIDTH), BF16),
            vmem((4, 640, 384), BF16),
            vmem((2, 640, 512), BF16),
            vmem((2, 4, 512, KV_WIDTH), BF16),
            vmem((128, 2560), BF16),
            vmem((2, 2, 128, 384), BF16),
            vmem((128, 384), BF16),
            vmem((512, 256), BF16),
            vmem((8, 512, 512), F32),
            vmem((512, 128), F32),
            vmem((4, 128, 128), F32),
            vmem((4, 128, 128), F32),
            vmem((4, 128, 128), F32),
            vmem((4, 128, 128), BF16),
            vmem((4, 8, 128), F32),
            vmem((4, 128, 128), BF16),
            vmem((4, 8, 128), F32),
            vmem((256, 512), BF16),
            vmem((4, 2, 160, 256), F32),
            vmem((4, 2, 160, 256), BF16),
            vmem((4, 160, 256), BF16),
            vmem((4, 160, 256), BF16),
            vmem((3, 160, 256), BF16),
            vmem((2, 160, 128), BF16),
            vmem((2, 160, 128), BF16),
            *ring,
            *ring,
            *ring,
            dma((4,)),
            dma((4,)),
            dma((3, 8)),
            dma((3, 8)),
            dma((17,)),
            dma((17,)),
        ],
        compiler_params=pltpu.CompilerParams(
            collective_id=0, has_side_effects=True, vmem_limit_bytes=56 * 1024 * 1024
        ),
        name="branch",
    )(
        tokens,
        raw_keys,
        raw_values,
        query_weight,
        output_weight.T,
        key_expand,
        key_mix,
        key_reduce.T,
        value_expand,
        value_mix,
        value_reduce,
    )
    return out.T


def solution(mesh):
    in_specs = (
        P("seq", None),
        P(SEQ_HEAD, None),
        P(SEQ_HEAD, None),
        P("seq", "head"),
        P("head", "seq"),
        P(),
        P(),
        P(),
        P(),
        P(),
        P(),
    )
    return jax.shard_map(
        shards, mesh=mesh, in_specs=in_specs, out_specs=P("seq", "head"), check_vma=False
    )
```

```python
import jax
import jax.numpy as jnp
from jax import lax
from jax.experimental import pallas as pl
from jax.experimental.pallas import tpu as pltpu
from jax.sharding import PartitionSpec as P

G = 4
BLK = 32
STRIDE = 16
CTX = 126976
DK = 192
DV = 128
KV_WIDTH = 384
SEQ_HEAD = ("seq", "head")
MESH = pl.DeviceIdType.MESH
BF16 = jnp.bfloat16
F32 = jnp.float32
EXP2_SCALE = DK**-0.5 * 1.4426950408889634


def compress_part(
    raw, edge, has_next, expands, starts, mix, reduce_weight, reduce_dim, order, moved, projected, hidden
):
    moved[0:256, :] = jnp.dot(order, raw[...], preferred_element_type=F32).astype(BF16)
    moved[256:272, :] = jnp.where(has_next, edge[...], jnp.zeros_like(edge))
    row = lax.broadcasted_iota(jnp.int32, (16, 768), 0)
    for group in range(G):
        expand = expands[group]
        start = starts[group]
        projected[...] = jnp.dot(
            moved[:, start : start + expand.shape[0]], expand, preferred_element_type=F32
        )
        first = jnp.zeros((16, 768), F32)
        second = jnp.zeros((16, 768), F32)
        for p in range(STRIDE):
            block = projected[16 * p : 16 * p + 16, :]
            first = first + block * mix[p : p + 1, :]
            second = second + block * mix[STRIDE + p : STRIDE + p + 1, :]
        beyond = jnp.sum(projected[256:272, :] * mix[STRIDE:, :], axis=0, keepdims=True)
        later = jnp.where(row == 15, beyond, pltpu.roll(second, 15, 0))
        hidden[16 * group : 16 * group + 16, :] = first + later
    value = hidden[...]
    activated = (0.5 * value * (1.0 + lax.erf(value * 0.5**0.5))).astype(BF16)
    return lax.dot_general(
        activated, reduce_weight[...], (((1,), (reduce_dim,)), ((), ())), preferred_element_type=F32
    ).astype(BF16)


class Place:
    def __init__(self):
        self.s = s = lax.axis_index("seq")
        self.h = h = lax.axis_index("head")
        self.y, self.z = s // 8, s % 8
        self.g, self.j = h // 4, h % 4
        self.core = h % 2
        self.x = (h // 2) % 4
        self.y_hi = h // 8
        self.parity = self.y % 2
        self.seq_pair = (self.y + 1 - 2 * self.parity) * 8 + self.z
        self.mate = h + 1 - 2 * self.core
        self.head_pair = h + 2 - 4 * ((h // 2) % 2)
        self.head_far = (h + 8) % 16
        self.right = self.y * 8 + (self.z + 1) % 8
        self.left = self.y * 8 + (self.z + 7) % 8

    def seq_at(self, y):
        return y * 8 + self.z


def remote(src, dst, send_sem, recv_sem, seq, head):
    return pltpu.make_async_remote_copy(
        src_ref=src,
        dst_ref=dst,
        send_sem=send_sem,
        recv_sem=recv_sem,
        device_id=(seq, head),
        device_id_type=MESH,
    )


class Gather:
    def __init__(self, at, buf, rows, streams, sems):
        self.at, self.buf, self.rows, self.streams = at, buf, rows, streams
        self.ys, self.yr, self.zs, self.zr = sems
        self.started = []

    def piece(self, i, z):
        start = pl.multiple_of(self.rows * z, 16)
        return self.buf.at[i, pl.ds(start, self.rows), :]

    def block(self, stream, z):
        first, count, _ = self.streams[stream]
        start = pl.multiple_of(self.rows * z, 16)
        return self.buf.at[pl.ds(first, count), pl.ds(start, self.rows), :]

    def y_copy(self, i, source):
        at = self.at
        target = (at.y + 4 - i) % 4
        return remote(
            source(target), self.piece(i, at.z), self.ys.at[i], self.yr.at[i], at.seq_at(target), at.h
        )

    def start_y(self, source):
        for i in (1, 2, 3):
            copy = self.y_copy(i, source)
            copy.start()
            self.started.append(copy)

    def first_z(self, source, streams):
        for stream in streams:
            first, count, _ = self.streams[stream]
            for i in range(first, first + count):
                if i > 0:
                    self.y_copy(i, source).wait_recv()
            self.send_z(stream, 1)

    def z_copy(self, way, stream, step, z):
        at = self.at
        block = self.block(stream, z)
        return remote(
            block,
            block,
            self.zs.at[way, stream, step - 1],
            self.zr.at[way, stream, step - 1],
            (at.right, at.left)[way],
            at.h,
        )

    def ways(self, stream, step):
        return (0, 1) if step < 4 else (self.streams[stream][2],)

    def send_z(self, stream, step):
        at = self.at
        for way in self.ways(stream, step):
            z = (at.z + 8 - (step - 1)) % 8 if way == 0 else (at.z + step - 1) % 8
            copy = self.z_copy(way, stream, step, z)
            copy.start()
            self.started.append(copy)

    def came_from(self, way, step):
        at = self.at
        return (at.z + 8 - step) % 8 if way == 0 else (at.z + step) % 8

    def wait_z(self, stream, step):
        for way in self.ways(stream, step):
            self.z_copy(way, stream, step, self.came_from(way, step)).wait_recv()

    def next_z(self, step):
        for stream in range(len(self.streams)):
            self.wait_z(stream, step - 1)
            self.send_z(stream, step)

    def end_z(self):
        for stream in range(len(self.streams)):
            self.wait_z(stream, 4)

    def finish_sends(self):
        for copy in self.started:
            copy.wait_send()


class HalfGather(Gather):
    def half_copy(self, n, source):
        at = self.at
        i = at.y % 2
        target = at.y // 2 + 2 * n
        return target, remote(
            source, self.piece(i, at.z), self.ys.at[n], self.yr.at[i], at.seq_at(target), at.h
        )

    def start_half(self, source):
        at = self.at
        for n in range(2):
            target, copy = self.half_copy(n, source)

            @pl.when(target != at.y)
            def _(copy=copy):
                copy.start()

            @pl.when(target == at.y)
            def _():
                start = pl.multiple_of(self.rows * at.z, 16)
                self.buf[at.y % 2, pl.ds(start, self.rows), :] = source[...]

    def wait_half(self, i, source):
        at = self.at
        origin = 2 * at.parity + i

        @pl.when(origin != at.y)
        def _():
            remote(
                source, self.piece(i, at.z), self.ys.at[i], self.yr.at[i], at.seq_at(origin), at.h
            ).wait_recv()

    def end_half(self, source):
        for n in range(2):
            target, copy = self.half_copy(n, source)

            @pl.when(target != self.at.y)
            def _(copy=copy):
                copy.wait_send()


QUARTERS = ((0, 1, 0), (1, 2, 1), (3, 1, 0))
HALVES = ((0, 1, 0), (1, 1, 1))


def attend_half(who, at, qbuf, stacked, kvb, scores, lane_max, store):
    for half in range(2):
        for head in range(2):
            rows = pl.ds((2 * half + head) * 128, 128)
            stacked[rows, 0:DK] = qbuf[who, half, :, head * DK : (head + 1) * DK]
    last = (3 + 4 - at.y) % 4
    first_position = CTX + at.s * 128
    half_index = (at.h // 2) % 2

    def entry(n):
        return n // 4, (last + n % 4) % 4

    def score_chunk(n, masked):
        quarter, i = entry(n)
        block = lax.dot_general(
            stacked[...], kvb[quarter, i, :, 0:256], (((1,), (1,)), ((), ())), preferred_element_type=F32
        )
        parts = [block[:, 128 * k : 128 * (k + 1)] for k in range(4)]
        if masked:
            column = lax.broadcasted_iota(jnp.int32, (512, 128), 1)
            row = lax.broadcasted_iota(jnp.int32, (512, 128), 0) % 128
            ids = 256 * (30 + column // 64) + 64 * (2 * half_index + quarter) + column % 64
            visible = STRIDE * ids + BLK - 1 <= first_position + row
            parts[3] = jnp.where(visible, parts[3], -jnp.inf)
        for k in range(4):
            scores[n, :, 128 * k : 128 * (k + 1)] = parts[k]
        return jnp.maximum(jnp.maximum(parts[0], parts[1]), jnp.maximum(parts[2], parts[3]))

    lane_max[...] = jnp.maximum(score_chunk(0, True), score_chunk(4, True))

    def other_chunk(n, carry):
        lane_max[...] = jnp.maximum(lane_max[...], score_chunk(n + n // 3 + 1, False))
        return carry

    lax.fori_loop(0, 6, other_chunk, 0, unroll=6)

    for head in range(4):
        rows = slice(head * 128, (head + 1) * 128)
        row_max = jnp.max(lane_max[rows, :], axis=1, keepdims=True)

        def weigh_chunk(n, carry):
            total, numerator = carry
            exponent = jnp.exp2((scores[n, rows, :] - row_max) * EXP2_SCALE)
            for k in range(4):
                total = total + exponent[:, 128 * k : 128 * (k + 1)]
            quarter, i = entry(n)
            numerator = numerator + jnp.dot(
                exponent.astype(BF16), kvb[quarter, i, :, 256:384], preferred_element_type=F32
            )
            return total, numerator

        start = jnp.zeros((128, 128), F32)
        total, numerator = lax.fori_loop(0, 8, weigh_chunk, (start, start), unroll=8)
        store(head, row_max, jnp.sum(total, axis=1, keepdims=True), numerator)


def kernel(
    tokens,
    raw_keys,
    raw_values,
    qw,
    ow,
    key_expand,
    key_mix,
    key_reduce,
    value_expand,
    value_mix,
    value_reduce,
    out,
    edge_keys,
    edge_values,
    moved_keys,
    moved_values,
    placed_expand,
    projected,
    hidden,
    kv4,
    qwb,
    owb,
    kvb,
    tokp,
    qbuf,
    qother,
    stacked,
    scores,
    lane_max,
    mine,
    mine_max,
    mine_total,
    part,
    stats,
    part_in,
    stats_in,
    attended,
    summed,
    o1,
    o1_in,
    o2,
    o2_in,
    o3,
    o3_in,
    q_ys, q_yr, q_zs, q_zr,
    k_ys, k_yr, k_zs, k_zr,
    o_ys, o_yr, o_zs, o_zr,
    r_s, r_r,
    m_s, m_r,
    e_s, e_r,
    t_s, t_r,
):
    at = Place()
    s, h, c = at.s, at.h, at.core

    barrier = pltpu.get_barrier_semaphore()
    partners = [(s, (h + d) % 16) for d in range(1, 16)]
    partners += [(at.seq_at((at.y + d) % 4), h) for d in (1, 2, 3)]
    partners += [(at.right, h), (at.left, h)]
    partners += [(at.seq_pair, at.head_pair), (at.seq_pair, at.head_far)]
    flat = 16 * s + h
    before, after = (flat + 511) % 512, (flat + 1) % 512
    partners += [(before // 16, before % 16), (after // 16, after % 16)]
    for partner in partners:
        pl.semaphore_signal(barrier, inc=1, device_id=partner, device_id_type=MESH)
    pl.semaphore_wait(barrier, len(partners))

    started = []

    def go(copy):
        copy.start()
        started.append(copy)
        return copy

    q = Gather(at, qwb, 80, QUARTERS, (q_ys, q_yr, q_zs, q_zr))
    o = HalfGather(at, owb, 80, HALVES, (o_ys, o_yr, o_zs, o_zr))
    k = Gather(at, kvb.at[c], 64, QUARTERS, (k_ys, k_yr, k_zs, k_zr))

    edge_in = [
        remote(source.at[0:16], target, e_s.at[i], e_r.at[i], before // 16, before % 16)
        for i, (source, target) in enumerate(((raw_keys, edge_keys), (raw_values, edge_values)), 11)
    ]
    for copy in edge_in:
        go(copy)

    def q_source(target):
        return qw.at[:, pl.ds(pl.multiple_of(384 * (target % 2), 128), 384)]

    qwb[0, pl.ds(pl.multiple_of(80 * at.z, 16), 80), :] = qw[
        :, pl.ds(pl.multiple_of(384 * at.parity, 128), 384)
    ]
    q.start_y(q_source)
    q.first_z(q_source, (0,))
    placed_expand[0, 0:DK, :] = key_expand[...]
    placed_expand[0, DK:256, :] = jnp.zeros((256 - DK, 768), BF16)
    placed_expand[1, 0 : 256 - DK, :] = jnp.zeros((256 - DK, 768), BF16)
    placed_expand[1, 256 - DK :, :] = key_expand[...]
    stacked[:, DK:] = jnp.zeros((512, 256 - DK), BF16)

    q.first_z(q_source, (1, 2))

    row = lax.broadcasted_iota(jnp.int32, (256, 256), 0)
    column = lax.broadcasted_iota(jnp.int32, (256, 256), 1)
    order = (column == 16 * (row % 16) + row // 16).astype(F32).astype(BF16)
    for copy in edge_in:
        copy.wait_recv()
    has_next = flat < 511
    packed_keys = compress_part(
        raw_keys,
        edge_keys,
        has_next,
        [placed_expand[group % 2] for group in range(G)],
        (0, 128, 384, 512),
        key_mix,
        key_reduce,
        1,
        order,
        moved_keys,
        projected,
        hidden,
    )
    packed_values = compress_part(
        raw_values,
        edge_values,
        has_next,
        [value_expand[...]] * G,
        (0, 128, 256, 384),
        value_mix,
        value_reduce,
        0,
        order,
        moved_values,
        projected,
        hidden,
    )
    for group in range(G):
        rows = slice(16 * group, 16 * group + 16)
        kv4[group, :, 0:DK] = packed_keys[rows, :]
        kv4[group, :, DK:256] = jnp.zeros((16, 256 - DK), BF16)
        kv4[group, :, 256:384] = packed_values[rows, :]

    own_rows = pl.ds(pl.multiple_of(64 * at.z + 16 * at.j, 16), 16)

    def spread_copy(group):
        quarter = at.g % 2
        return remote(
            kv4.at[group],
            kvb.at[quarter, 0, own_rows, :],
            r_s.at[group],
            r_r.at[at.j],
            s,
            4 * group + at.g,
        )

    for group in range(G):
        @pl.when(4 * group + at.g != h)
        def _(group=group):
            spread_copy(group).start()

        @pl.when(4 * group + at.g == h)
        def _(group=group):
            kvb[c, 0, own_rows, :] = kv4[group]

    def k_source(target):
        return k.piece(0, at.z)

    def mate_copy(quarter, stream, index, z):
        first, count, _ = QUARTERS[stream]
        start = pl.multiple_of(64 * z, 16)
        block = kvb.at[quarter, pl.ds(first, count), pl.ds(start, 64), :]
        return remote(
            block, block, m_s.at[stream, index], m_r.at[stream, index], s, at.mate
        )

    def k_arrived(stream, step):
        k.wait_z(stream, step)
        for way in k.ways(stream, step):
            index = 7 if step == 4 else 3 * way + step
            go(mate_copy(c, stream, index, k.came_from(way, step)))

    def k_round(step):
        for stream in (0, 1, 2):
            k_arrived(stream, step - 1)
            k.send_z(stream, step)

    q.next_z(2)
    for m in range(4):
        @pl.when(4 * at.j + m != h)
        def _(m=m):
            rows = pl.ds(pl.multiple_of(64 * at.z + 16 * m, 16), 16)
            remote(
                kv4.at[0], kvb.at[c, 0, rows, :], r_s.at[0], r_r.at[m], s, 4 * at.j + m
            ).wait_recv()
    k.start_y(k_source)
    half_tokens = pl.ds(pl.multiple_of(1280 * c, 128), 1280)
    tok_copy = go(
        remote(
            tokens.at[:, half_tokens], tokp.at[:, half_tokens], e_s.at[0], e_r.at[0], at.seq_pair, h
        )
    )
    o.start_half(ow)
    k.first_z(k_source, (0,))
    go(mate_copy(c, 0, 0, at.z))
    q.next_z(3)
    for stream in (1, 2):
        k.first_z(k_source, (stream,))
        go(mate_copy(c, stream, 0, at.z))
    q.next_z(4)
    k_round(2)
    tok_copy.wait_recv()
    arrived_tokens = tokp.at[:, half_tokens]
    go(remote(arrived_tokens, arrived_tokens, e_s.at[13], e_r.at[13], s, at.mate))
    q.end_z()
    other_half = tokp.at[:, pl.ds(pl.multiple_of(1280 - 1280 * c, 128), 1280)]
    remote(other_half, other_half, e_s.at[13], e_r.at[13], s, at.mate).wait_recv()

    def project_queries(source):
        total = jnp.zeros((128, 384), F32)
        for i in range(4):
            start = pl.multiple_of(640 * ((at.y + i) % 4), 128)
            total = total + jnp.dot(
                source[:, pl.ds(start, 640)], qwb[i], preferred_element_type=F32
            )
        return total.astype(BF16)

    qother[...] = project_queries(tokp)
    q_in = [
        remote(qother, qbuf.at[0, at.parity], e_s.at[1], e_r.at[1], at.seq_pair, h),
        remote(qother, qbuf.at[1, at.parity], e_s.at[2], e_r.at[2], at.seq_pair, at.head_pair),
    ]
    go(q_in[0])
    go(q_in[1])
    qbuf[0, at.parity] = project_queries(tokens)
    q_in.append(
        go(
            remote(
                qbuf.at[0, at.parity], qbuf.at[1, at.parity], e_s.at[3], e_r.at[3], s, at.head_pair
            )
        )
    )
    k_round(3)
    for i in (0, 1):
        o.wait_half(i, ow)
        o.send_z(i, 1)
    k_round(4)
    o.next_z(2)
    for stream in (0, 1, 2):
        k_arrived(stream, 4)
    q_in[0].wait_recv()
    q_in[2].wait_recv()
    q_in[1].wait_recv()
    for stream in (0, 1, 2):
        mate_copy(1 - c, stream, 0, at.z).wait_recv()
        for step in (1, 2, 3, 4):
            for way in k.ways(stream, step):
                index = 7 if step == 4 else 3 * way + step
                mate_copy(1 - c, stream, index, k.came_from(way, step)).wait_recv()

    lane = lax.broadcasted_iota(jnp.int32, (128, 128), 1)

    def store_part(head, row_max, row_total, numerator):
        part[head] = numerator.astype(BF16)
        tile = jnp.where(lane == 0, row_max, jnp.where(lane == 1, row_total, 0.0))
        stats[head] = jnp.transpose(tile)[0:8, :]

    attend_half(1, at, qbuf, stacked, kvb, scores, lane_max, store_part)
    part_copy = go(remote(part, part_in, e_s.at[4], e_r.at[4], s, at.head_pair))
    stat_copy = go(remote(stats, stats_in, e_s.at[5], e_r.at[5], s, at.head_pair))
    o.next_z(3)

    def store_mine(head, row_max, row_total, numerator):
        mine[head] = numerator
        mine_max[head] = jnp.broadcast_to(row_max, (128, 128))
        mine_total[head] = jnp.broadcast_to(row_total, (128, 128))

    attend_half(0, at, qbuf, stacked, kvb, scores, lane_max, store_mine)
    part_copy.wait_recv()
    stat_copy.wait_recv()
    for head in range(4):
        tile = jnp.concatenate([stats_in[head], jnp.zeros((120, 128), F32)], axis=0)
        tile = jnp.transpose(tile)
        other_max = jnp.broadcast_to(tile[:, 0:1], (128, 128))
        other_total = jnp.broadcast_to(tile[:, 1:2], (128, 128))
        top = jnp.maximum(mine_max[head], other_max)
        own_part = jnp.exp2((mine_max[head] - top) * EXP2_SCALE)
        other_part = jnp.exp2((other_max - top) * EXP2_SCALE)
        total = mine_total[head] * own_part + other_total * other_part
        value = mine[head] * own_part + part_in[head].astype(F32) * other_part
        attended[0:128, head * DV : (head + 1) * DV] = (value / total).astype(BF16)
    attended_copy = go(
        remote(
            attended.at[0:128], attended.at[128:256], e_s.at[6], e_r.at[6], at.seq_pair, h
        )
    )
    o.next_z(4)
    o.end_z()

    mate_sums = []
    for n in range(2):
        if n == 1:
            attended_copy.wait_recv()
        for i in range(2):
            block = lax.dot_general(
                owb[i],
                attended[128 * n : 128 * (n + 1)],
                (((1,), (1,)), ((), ())),
                preferred_element_type=F32,
            ).reshape(2, 2, 160, 128)
            summed[n, 2 * i : 2 * i + 2] = block
            o1[n, 2 * i : 2 * i + 2] = block.astype(BF16)
        mate_sums.append(
            go(remote(o1.at[n, :, 1 - c], o1_in.at[n], t_s.at[n, 0], t_r.at[n, 0], s, at.mate))
        )
    x_sums = [[], []]
    for n in range(2):
        mate_sums[n].wait_recv()
        for x in range(4):
            summed[n, x, 0] = summed[n, x, c] + o1_in[n, x].astype(F32)
            o2[n, x] = summed[n, x, 0].astype(BF16)
        for d in (1, 2, 3):
            x = (at.x + d) % 4
            target = 8 * at.y_hi + 2 * x + c
            x_sums[n].append(
                go(remote(o2.at[n, x], o2_in.at[n, d - 1], t_s.at[n, d], t_r.at[n, d], s, target))
            )

    def x_total(n):
        for copy in x_sums[n]:
            copy.wait_recv()
        value = summed[n, at.x, 0]
        for d in range(3):
            value = value + o2_in[n, d].astype(F32)
        return value

    final_here = at.y_hi == at.parity
    own_sum = remote(o3.at[0], o3_in.at[1], t_s.at[0, 4], t_r.at[0, 4], s, at.head_far)
    cross_sum = remote(o3.at[1], o3_in.at[1], t_s.at[1, 4], t_r.at[0, 4], at.seq_pair, at.head_far)
    pair_sum = remote(o3.at[1], o3_in.at[0], t_s.at[1, 4], t_r.at[1, 4], at.seq_pair, h)
    own = x_total(0)
    o3[0] = own.astype(BF16)

    @pl.when(jnp.logical_not(final_here))
    def _():
        own_sum.start()

    o3[1] = x_total(1).astype(BF16)

    @pl.when(final_here)
    def _():
        pair_sum.start()
        own_sum.wait_recv()
        out[...] = (own + o3_in[1].astype(F32)).astype(BF16)
        pair_sum.wait_send()

    @pl.when(jnp.logical_not(final_here))
    def _():
        cross_sum.start()
        pair_sum.wait_recv()
        cross_sum.wait_recv()
        out[...] = (o3_in[0].astype(F32) + o3_in[1].astype(F32)).astype(BF16)
        cross_sum.wait_send()
        own_sum.wait_send()

    for copy in started:
        copy.wait_send()
    for gather in (q, k, o):
        gather.finish_sends()
    o.end_half(ow)
    for group in range(G):
        @pl.when(4 * group + at.g != h)
        def _(group=group):
            spread_copy(group).wait_send()


def shards(
    tokens,
    raw_keys,
    raw_values,
    query_weight,
    output_weight,
    key_expand,
    key_mix,
    key_reduce,
    value_expand,
    value_mix,
    value_reduce,
):
    vmem = pltpu.VMEM
    dma = pltpu.SemaphoreType.DMA
    ring = [dma((4,)), dma((4,)), dma((2, 3, 4)), dma((2, 3, 4))]
    out = pl.pallas_call(
        kernel,
        out_shape=jax.ShapeDtypeStruct((160, 128), BF16),
        in_specs=[pl.BlockSpec(memory_space=vmem)] * 11,
        out_specs=pl.BlockSpec(memory_space=vmem),
        scratch_shapes=[
            vmem((16, 768), BF16),
            vmem((16, 512), BF16),
            vmem((272, 768), BF16),
            vmem((272, 512), BF16),
            vmem((2, 256, 768), BF16),
            vmem((272, 768), F32),
            vmem((64, 768), F32),
            vmem((G, 16, KV_WIDTH), BF16),
            vmem((4, 640, 384), BF16),
            vmem((2, 640, 512), BF16),
            vmem((2, 4, 512, KV_WIDTH), BF16),
            vmem((128, 2560), BF16),
            vmem((2, 2, 128, 384), BF16),
            vmem((128, 384), BF16),
            vmem((512, 256), BF16),
            vmem((8, 512, 512), F32),
            vmem((512, 128), F32),
            vmem((4, 128, 128), F32),
            vmem((4, 128, 128), F32),
            vmem((4, 128, 128), F32),
            vmem((4, 128, 128), BF16),
            vmem((4, 8, 128), F32),
            vmem((4, 128, 128), BF16),
            vmem((4, 8, 128), F32),
            vmem((256, 512), BF16),
            vmem((2, 4, 2, 160, 128), F32),
            vmem((2, 4, 2, 160, 128), BF16),
            vmem((2, 4, 160, 128), BF16),
            vmem((2, 4, 160, 128), BF16),
            vmem((2, 3, 160, 128), BF16),
            vmem((2, 160, 128), BF16),
            vmem((2, 160, 128), BF16),
            *ring,
            *ring,
            *ring,
            dma((4,)),
            dma((4,)),
            dma((3, 8)),
            dma((3, 8)),
            dma((14,)),
            dma((14,)),
            dma((2, 5)),
            dma((2, 5)),
        ],
        compiler_params=pltpu.CompilerParams(
            collective_id=0, has_side_effects=True, vmem_limit_bytes=56 * 1024 * 1024
        ),
        name="branch",
    )(
        tokens,
        raw_keys,
        raw_values,
        query_weight,
        output_weight.T,
        key_expand,
        key_mix,
        key_reduce.T,
        value_expand,
        value_mix,
        value_reduce,
    )
    return out.T


def solution(mesh):
    in_specs = (
        P("seq", None),
        P(SEQ_HEAD, None),
        P(SEQ_HEAD, None),
        P("seq", "head"),
        P("head", "seq"),
        P(),
        P(),
        P(),
        P(),
        P(),
        P(),
    )
    return jax.shard_map(
        shards, mesh=mesh, in_specs=in_specs, out_specs=P("seq", "head"), check_vma=False
    )
```

```python
import jax
import jax.numpy as jnp
from jax import lax
from jax.experimental import pallas as pl
from jax.experimental.pallas import tpu as pltpu
from jax.sharding import PartitionSpec as P

G = 4
BLK = 32
STRIDE = 16
CTX = 126976
DK = 192
DV = 128
SEQ_HEAD = ("seq", "head")
MESH = pl.DeviceIdType.MESH
BF16 = jnp.bfloat16
F32 = jnp.float32
EXP2_SCALE = DK**-0.5 * 1.4426950408889634


def compress_part(
    raw, edge, has_next, expands, starts, mix, reduce_weight, reduce_dim, order, moved, projected, hidden
):
    moved[0:256, :] = jnp.dot(order, raw[...], preferred_element_type=F32).astype(BF16)
    moved[256:272, :] = jnp.where(has_next, edge[...], jnp.zeros_like(edge))
    row = lax.broadcasted_iota(jnp.int32, (16, 768), 0)
    for group in range(G):
        expand = expands[group]
        start = starts[group]
        projected[...] = jnp.dot(
            moved[:, start : start + expand.shape[0]], expand, preferred_element_type=F32
        )
        first = jnp.zeros((16, 768), F32)
        second = jnp.zeros((16, 768), F32)
        for p in range(STRIDE):
            block = projected[16 * p : 16 * p + 16, :]
            first = first + block * mix[p : p + 1, :]
            second = second + block * mix[STRIDE + p : STRIDE + p + 1, :]
        beyond = jnp.sum(projected[256:272, :] * mix[STRIDE:, :], axis=0, keepdims=True)
        later = jnp.where(row == 15, beyond, pltpu.roll(second, 15, 0))
        hidden[16 * group : 16 * group + 16, :] = first + later
    value = hidden[...]
    activated = (0.5 * value * (1.0 + lax.erf(value * 0.5**0.5))).astype(BF16)
    return lax.dot_general(
        activated, reduce_weight[...], (((1,), (reduce_dim,)), ((), ())), preferred_element_type=F32
    ).astype(BF16)


class Place:
    def __init__(self):
        self.s = s = lax.axis_index("seq")
        self.h = h = lax.axis_index("head")
        self.y, self.z = s // 8, s % 8
        self.g, self.j = h // 4, h % 4
        self.core = h % 2
        self.x = (h // 2) % 4
        self.y_hi = h // 8
        self.parity = self.y % 2
        self.seq_pair = (self.y + 1 - 2 * self.parity) * 8 + self.z
        self.mate = h + 1 - 2 * self.core
        self.head_pair = h + 2 - 4 * ((h // 2) % 2)
        self.head_far = (h + 8) % 16
        self.right = self.y * 8 + (self.z + 1) % 8
        self.left = self.y * 8 + (self.z + 7) % 8

    def seq_at(self, y):
        return y * 8 + self.z


def remote(src, dst, send_sem, recv_sem, seq, head):
    return pltpu.make_async_remote_copy(
        src_ref=src,
        dst_ref=dst,
        send_sem=send_sem,
        recv_sem=recv_sem,
        device_id=(seq, head),
        device_id_type=MESH,
    )


class Gather:
    def __init__(self, at, buf, rows, streams, sems):
        self.at, self.buf, self.rows, self.streams = at, buf, rows, streams
        self.ys, self.yr, self.zs, self.zr = sems
        self.started = []

    def piece(self, i, z):
        start = pl.multiple_of(self.rows * z, 16)
        return self.buf.at[i, pl.ds(start, self.rows), :]

    def block(self, stream, z):
        first, count, _ = self.streams[stream]
        start = pl.multiple_of(self.rows * z, 16)
        return self.buf.at[pl.ds(first, count), pl.ds(start, self.rows), :]

    def y_copy(self, i, source):
        at = self.at
        target = (at.y + 4 - i) % 4
        return remote(
            source(target), self.piece(i, at.z), self.ys.at[i], self.yr.at[i], at.seq_at(target), at.h
        )

    def start_y(self, source):
        for i in (1, 2, 3):
            copy = self.y_copy(i, source)
            copy.start()
            self.started.append(copy)

    def first_z(self, source, streams):
        for stream in streams:
            first, count, _ = self.streams[stream]
            for i in range(first, first + count):
                if i > 0:
                    self.y_copy(i, source).wait_recv()
            self.send_z(stream, 1)

    def z_copy(self, way, stream, step, z):
        at = self.at
        block = self.block(stream, z)
        return remote(
            block,
            block,
            self.zs.at[way, stream, step - 1],
            self.zr.at[way, stream, step - 1],
            (at.right, at.left)[way],
            at.h,
        )

    def ways(self, stream, step):
        return (0, 1) if step < 4 else (self.streams[stream][2],)

    def send_z(self, stream, step):
        at = self.at
        for way in self.ways(stream, step):
            z = (at.z + 8 - (step - 1)) % 8 if way == 0 else (at.z + step - 1) % 8
            copy = self.z_copy(way, stream, step, z)
            copy.start()
            self.started.append(copy)

    def came_from(self, way, step):
        at = self.at
        return (at.z + 8 - step) % 8 if way == 0 else (at.z + step) % 8

    def wait_z(self, stream, step):
        for way in self.ways(stream, step):
            self.z_copy(way, stream, step, self.came_from(way, step)).wait_recv()

    def next_z(self, step):
        for stream in range(len(self.streams)):
            self.wait_z(stream, step - 1)
            self.send_z(stream, step)

    def end_z(self):
        for stream in range(len(self.streams)):
            self.wait_z(stream, 4)

    def finish_sends(self):
        for copy in self.started:
            copy.wait_send()


class HalfGather(Gather):
    def half_copy(self, n, source):
        at = self.at
        i = at.y % 2
        target = at.y // 2 + 2 * n
        return target, remote(
            source, self.piece(i, at.z), self.ys.at[n], self.yr.at[i], at.seq_at(target), at.h
        )

    def start_half(self, source):
        at = self.at
        for n in range(2):
            target, copy = self.half_copy(n, source)

            @pl.when(target != at.y)
            def _(copy=copy):
                copy.start()

            @pl.when(target == at.y)
            def _():
                start = pl.multiple_of(self.rows * at.z, 16)
                self.buf[at.y % 2, pl.ds(start, self.rows), :] = source[...]

    def wait_half(self, i, source):
        at = self.at
        origin = 2 * at.parity + i

        @pl.when(origin != at.y)
        def _():
            remote(
                source, self.piece(i, at.z), self.ys.at[i], self.yr.at[i], at.seq_at(origin), at.h
            ).wait_recv()

    def end_half(self, source):
        for n in range(2):
            target, copy = self.half_copy(n, source)

            @pl.when(target != self.at.y)
            def _(copy=copy):
                copy.wait_send()


QUARTERS = ((0, 1, 0), (1, 2, 1), (3, 1, 0))
HALVES = ((0, 1, 0), (1, 1, 1))


def attend_half(who, at, qbuf, stacked, kvb, scores, lane_max, store, hooks):
    for half in range(2):
        for head in range(2):
            rows = pl.ds((2 * half + head) * 128, 128)
            queries = qbuf[who, half, :, head * DK : (head + 1) * DK]
            stacked[0, rows, 0:DK] = queries
            stacked[1, rows, 0:128] = queries[:, 0:128]
            stacked[1, rows, DK:256] = queries[:, 128:DK]
    last = (3 + 4 - at.y) % 4
    first_position = CTX + at.s * 128
    half_index = (at.h // 2) % 2

    def entry(n):
        return (at.core + n // 4) % 2, (last + n % 4) % 4

    def rows_of(n, start):
        quarter, i = entry(n)
        return kvb[quarter, i].reshape(8, 160, 128)[:, start : start + 32].reshape(256, 128)

    def score_chunk(n, masked):
        quarter, _ = entry(n)
        upper = rows_of(n, 128)
        parts = []
        for side in range(2):
            keys = jnp.concatenate([rows_of(n, 32 * side), upper], axis=1)
            block = lax.dot_general(
                stacked[side], keys, (((1,), (1,)), ((), ())), preferred_element_type=F32
            )
            parts.append(block[:, 0:128])
            tail = block[:, 128:256]
            if masked:
                column = lax.broadcasted_iota(jnp.int32, (512, 128), 1)
                row = lax.broadcasted_iota(jnp.int32, (512, 128), 0) % 128
                ids = 256 * (28 + column // 32) + 64 * (2 * half_index + quarter)
                ids = ids + 32 * side + column % 32
                visible = STRIDE * ids + BLK - 1 <= first_position + row
                tail = jnp.where(visible, tail, -jnp.inf)
            parts.append(tail)
        for k in range(4):
            scores[n, :, 128 * k : 128 * (k + 1)] = parts[k]
        return jnp.maximum(jnp.maximum(parts[0], parts[1]), jnp.maximum(parts[2], parts[3]))

    lane_max[...] = score_chunk(0, True)
    for n in (1, 2, 3):
        lane_max[...] = jnp.maximum(lane_max[...], score_chunk(n, False))
    hooks[0]()
    lane_max[...] = jnp.maximum(lane_max[...], score_chunk(4, True))
    for n in (5, 6, 7):
        lane_max[...] = jnp.maximum(lane_max[...], score_chunk(n, False))
    hooks[1]()

    for head in range(4):
        rows = slice(head * 128, (head + 1) * 128)
        row_max = jnp.max(lane_max[rows, :], axis=1, keepdims=True)
        total = jnp.zeros((128, 128), F32)
        numerator = jnp.zeros((128, 128), F32)
        for n in range(8):
            exponent = jnp.exp2((scores[n, rows, :] - row_max) * EXP2_SCALE)
            for k in range(4):
                total = total + exponent[:, 128 * k : 128 * (k + 1)]
            values = jnp.concatenate([rows_of(n, 64), rows_of(n, 96)], axis=0)
            numerator = numerator + jnp.dot(
                exponent.astype(BF16), values, preferred_element_type=F32
            )
        store(head, row_max, jnp.sum(total, axis=1, keepdims=True), numerator)


def kernel(
    tokens,
    raw_keys,
    raw_values,
    qw,
    ow,
    key_expand,
    key_mix,
    key_reduce,
    value_expand,
    value_mix,
    value_reduce,
    out,
    edge_keys,
    edge_values,
    moved_keys,
    moved_values,
    placed_expand,
    projected,
    hidden,
    kv4,
    kvt,
    qwb,
    owb,
    kvb,
    tokp,
    qbuf,
    qother,
    stacked,
    scores,
    lane_max,
    mine,
    mine_max,
    mine_total,
    part,
    stats,
    part_in,
    stats_in,
    attended,
    summed,
    o1,
    o1_in,
    o2,
    o2_in,
    o3,
    o3_in,
    q_ys, q_yr, q_zs, q_zr,
    k_ys, k_yr, k_zs, k_zr,
    o_ys, o_yr, o_zs, o_zr,
    r_s, r_r,
    m_s, m_r,
    e_s, e_r,
    t_s, t_r,
):
    at = Place()
    s, h, c = at.s, at.h, at.core

    barrier = pltpu.get_barrier_semaphore()
    partners = [(s, (h + d) % 16) for d in range(1, 16)]
    partners += [(at.seq_at((at.y + d) % 4), h) for d in (1, 2, 3)]
    partners += [(at.right, h), (at.left, h)]
    partners += [(at.seq_pair, at.head_pair), (at.seq_pair, at.head_far)]
    flat = 16 * s + h
    before, after = (flat + 511) % 512, (flat + 1) % 512
    partners += [(before // 16, before % 16), (after // 16, after % 16)]
    for partner in partners:
        pl.semaphore_signal(barrier, inc=1, device_id=partner, device_id_type=MESH)
    pl.semaphore_wait(barrier, len(partners))

    started = []

    def go(copy):
        copy.start()
        started.append(copy)
        return copy

    q = Gather(at, qwb, 80, QUARTERS, (q_ys, q_yr, q_zs, q_zr))
    o = HalfGather(at, owb, 80, HALVES, (o_ys, o_yr, o_zs, o_zr))
    k = Gather(at, kvb.at[c], 160, QUARTERS, (k_ys, k_yr, k_zs, k_zr))

    edge_in = [
        remote(source.at[0:16], target, e_s.at[i], e_r.at[i], before // 16, before % 16)
        for i, (source, target) in enumerate(((raw_keys, edge_keys), (raw_values, edge_values)), 11)
    ]
    for copy in edge_in:
        go(copy)

    def q_source(target):
        return qw.at[:, pl.ds(pl.multiple_of(384 * (target % 2), 128), 384)]

    qwb[0, pl.ds(pl.multiple_of(80 * at.z, 16), 80), :] = qw[
        :, pl.ds(pl.multiple_of(384 * at.parity, 128), 384)
    ]
    q.start_y(q_source)
    q.first_z(q_source, (0,))
    placed_expand[0, 0:DK, :] = key_expand[...]
    placed_expand[0, DK:256, :] = jnp.zeros((256 - DK, 768), BF16)
    placed_expand[1, 0 : 256 - DK, :] = jnp.zeros((256 - DK, 768), BF16)
    placed_expand[1, 256 - DK :, :] = key_expand[...]
    stacked[0, :, DK:] = jnp.zeros((512, 256 - DK), BF16)
    stacked[1, :, 128:DK] = jnp.zeros((512, DK - 128), BF16)

    q.first_z(q_source, (1, 2))

    row = lax.broadcasted_iota(jnp.int32, (256, 256), 0)
    column = lax.broadcasted_iota(jnp.int32, (256, 256), 1)
    order = (column == 16 * (row % 16) + row // 16).astype(F32).astype(BF16)
    for copy in edge_in:
        copy.wait_recv()
    has_next = flat < 511
    packed_keys = compress_part(
        raw_keys,
        edge_keys,
        has_next,
        [placed_expand[group % 2] for group in range(G)],
        (0, 128, 384, 512),
        key_mix,
        key_reduce,
        1,
        order,
        moved_keys,
        projected,
        hidden,
    )
    packed_values = compress_part(
        raw_values,
        edge_values,
        has_next,
        [value_expand[...]] * G,
        (0, 128, 256, 384),
        value_mix,
        value_reduce,
        0,
        order,
        moved_values,
        projected,
        hidden,
    )
    for group in range(G):
        rows = slice(16 * group, 16 * group + 16)
        kv4[group, 0:16, :] = packed_keys[rows, 0:128]
        kv4[group, 16:32, :] = packed_values[rows, :]
        kv4[group, 32:48, 0:64] = packed_keys[rows, 128:DK]
        kv4[group, 32:48, 64:128] = packed_keys[rows, 128:DK]

    def spread_copy(group):
        return remote(kv4.at[group], kvt.at[at.j], r_s.at[group], r_r.at[at.j], s, 4 * group + at.g)

    for group in range(G):
        @pl.when(4 * group + at.g != h)
        def _(group=group):
            spread_copy(group).start()

        @pl.when(4 * group + at.g == h)
        def _(group=group):
            kvt[at.j] = kv4[group]

    def k_source(target):
        return k.piece(0, at.z)

    def mate_copy(quarter, stream, index, z):
        first, count, _ = QUARTERS[stream]
        start = pl.multiple_of(160 * z, 16)
        block = kvb.at[quarter, pl.ds(first, count), pl.ds(start, 160), :]
        return remote(
            block, block, m_s.at[stream, index], m_r.at[stream, index], s, at.mate
        )

    def k_arrived(stream, step):
        k.wait_z(stream, step)
        for way in k.ways(stream, step):
            index = 7 if step == 4 else 3 * way + step
            go(mate_copy(c, stream, index, k.came_from(way, step)))

    def k_round(step):
        for stream in (0, 1, 2):
            k_arrived(stream, step - 1)
            k.send_z(stream, step)

    q.next_z(2)
    for m in range(4):
        @pl.when(4 * at.j + m != h)
        def _(m=m):
            remote(
                kv4.at[0], kvt.at[m], r_s.at[0], r_r.at[m], s, 4 * at.j + m
            ).wait_recv()
    piece = pl.multiple_of(160 * at.z, 16)
    left_lanes = lax.broadcasted_iota(jnp.int32, (16, 128), 1) < 64
    for m in range(4):
        kvb[c, 0, pl.ds(piece + 16 * m, 16), :] = kvt[m, 0:16, :]
        kvb[c, 0, pl.ds(piece + 64 + 16 * m, 16), :] = kvt[m, 16:32, :]
    for m in range(2):
        both = jnp.where(
            left_lanes, kvt[m, 32:48, :].astype(F32), kvt[m + 2, 32:48, :].astype(F32)
        )
        kvb[c, 0, pl.ds(piece + 128 + 16 * m, 16), :] = both.astype(BF16)
    k.start_y(k_source)
    half_tokens = pl.ds(pl.multiple_of(1280 * c, 128), 1280)
    tok_copy = go(
        remote(
            tokens.at[:, half_tokens], tokp.at[:, half_tokens], e_s.at[0], e_r.at[0], at.seq_pair, h
        )
    )
    o.start_half(ow)
    k.first_z(k_source, (0,))
    go(mate_copy(c, 0, 0, at.z))
    q.next_z(3)
    for stream in (1, 2):
        k.first_z(k_source, (stream,))
        go(mate_copy(c, stream, 0, at.z))
    q.next_z(4)
    k_round(2)
    tok_copy.wait_recv()
    arrived_tokens = tokp.at[:, half_tokens]
    go(remote(arrived_tokens, arrived_tokens, e_s.at[13], e_r.at[13], s, at.mate))
    q.end_z()
    other_half = tokp.at[:, pl.ds(pl.multiple_of(1280 - 1280 * c, 128), 1280)]
    remote(other_half, other_half, e_s.at[13], e_r.at[13], s, at.mate).wait_recv()

    def project_queries(source):
        total = jnp.zeros((128, 384), F32)
        for i in range(4):
            start = pl.multiple_of(640 * ((at.y + i) % 4), 128)
            total = total + jnp.dot(
                source[:, pl.ds(start, 640)], qwb[i], preferred_element_type=F32
            )
        return total.astype(BF16)

    qother[...] = project_queries(tokp)
    q_in = [
        remote(qother, qbuf.at[0, at.parity], e_s.at[1], e_r.at[1], at.seq_pair, h),
        remote(qother, qbuf.at[1, at.parity], e_s.at[2], e_r.at[2], at.seq_pair, at.head_pair),
    ]
    go(q_in[0])
    go(q_in[1])
    qbuf[0, at.parity] = project_queries(tokens)
    q_in.append(
        go(
            remote(
                qbuf.at[0, at.parity], qbuf.at[1, at.parity], e_s.at[3], e_r.at[3], s, at.head_pair
            )
        )
    )
    k_round(3)
    for i in (0, 1):
        o.wait_half(i, ow)
        o.send_z(i, 1)
    k_round(4)
    o.next_z(2)
    for stream in (0, 1, 2):
        k_arrived(stream, 4)
    q_in[0].wait_recv()
    q_in[2].wait_recv()
    q_in[1].wait_recv()
    def mate_arrived():
        for stream in (0, 1, 2):
            mate_copy(1 - c, stream, 0, at.z).wait_recv()
            for step in (1, 2, 3, 4):
                for way in k.ways(stream, step):
                    index = 7 if step == 4 else 3 * way + step
                    mate_copy(1 - c, stream, index, k.came_from(way, step)).wait_recv()

    def nothing():
        pass

    lane = lax.broadcasted_iota(jnp.int32, (128, 128), 1)

    def store_part(head, row_max, row_total, numerator):
        part[head] = numerator.astype(BF16)
        tile = jnp.where(lane == 0, row_max, jnp.where(lane == 1, row_total, 0.0))
        stats[head] = jnp.transpose(tile)[0:8, :]

    attend_half(1, at, qbuf, stacked, kvb, scores, lane_max, store_part, (mate_arrived, lambda: o.next_z(3)))
    part_copy = go(remote(part, part_in, e_s.at[4], e_r.at[4], s, at.head_pair))
    stat_copy = go(remote(stats, stats_in, e_s.at[5], e_r.at[5], s, at.head_pair))

    def store_mine(head, row_max, row_total, numerator):
        mine[head] = numerator
        mine_max[head] = jnp.broadcast_to(row_max, (128, 128))
        mine_total[head] = jnp.broadcast_to(row_total, (128, 128))

    attend_half(0, at, qbuf, stacked, kvb, scores, lane_max, store_mine, (nothing, lambda: o.next_z(4)))
    part_copy.wait_recv()
    stat_copy.wait_recv()
    for head in range(4):
        tile = jnp.concatenate([stats_in[head], jnp.zeros((120, 128), F32)], axis=0)
        tile = jnp.transpose(tile)
        other_max = jnp.broadcast_to(tile[:, 0:1], (128, 128))
        other_total = jnp.broadcast_to(tile[:, 1:2], (128, 128))
        top = jnp.maximum(mine_max[head], other_max)
        own_part = jnp.exp2((mine_max[head] - top) * EXP2_SCALE)
        other_part = jnp.exp2((other_max - top) * EXP2_SCALE)
        total = mine_total[head] * own_part + other_total * other_part
        value = mine[head] * own_part + part_in[head].astype(F32) * other_part
        attended[0:128, head * DV : (head + 1) * DV] = (value / total).astype(BF16)
    attended_copy = go(
        remote(
            attended.at[0:128], attended.at[128:256], e_s.at[6], e_r.at[6], at.seq_pair, h
        )
    )
    o.end_z()

    mate_sums = []
    for n in range(2):
        if n == 1:
            attended_copy.wait_recv()
        for i in range(2):
            block = lax.dot_general(
                owb[i],
                attended[128 * n : 128 * (n + 1)],
                (((1,), (1,)), ((), ())),
                preferred_element_type=F32,
            ).reshape(2, 2, 160, 128)
            summed[n, 2 * i : 2 * i + 2] = block
            o1[n, 2 * i : 2 * i + 2] = block.astype(BF16)
        mate_sums.append(
            go(remote(o1.at[n, :, 1 - c], o1_in.at[n], t_s.at[n, 0], t_r.at[n, 0], s, at.mate))
        )
    x_sums = [[], []]
    for n in range(2):
        mate_sums[n].wait_recv()
        for x in range(4):
            summed[n, x, 0] = summed[n, x, c] + o1_in[n, x].astype(F32)
            o2[n, x] = summed[n, x, 0].astype(BF16)
        for d in (1, 2, 3):
            x = (at.x + d) % 4
            target = 8 * at.y_hi + 2 * x + c
            x_sums[n].append(
                go(remote(o2.at[n, x], o2_in.at[n, d - 1], t_s.at[n, d], t_r.at[n, d], s, target))
            )

    def x_total(n):
        for copy in x_sums[n]:
            copy.wait_recv()
        value = summed[n, at.x, 0]
        for d in range(3):
            value = value + o2_in[n, d].astype(F32)
        return value

    final_here = at.y_hi == at.parity
    own_sum = remote(o3.at[0], o3_in.at[1], t_s.at[0, 4], t_r.at[0, 4], s, at.head_far)
    cross_sum = remote(o3.at[1], o3_in.at[1], t_s.at[1, 4], t_r.at[0, 4], at.seq_pair, at.head_far)
    pair_sum = remote(o3.at[1], o3_in.at[0], t_s.at[1, 4], t_r.at[1, 4], at.seq_pair, h)
    own = x_total(0)
    o3[0] = own.astype(BF16)

    @pl.when(jnp.logical_not(final_here))
    def _():
        own_sum.start()

    o3[1] = x_total(1).astype(BF16)

    @pl.when(final_here)
    def _():
        pair_sum.start()
        own_sum.wait_recv()
        out[...] = (own + o3_in[1].astype(F32)).astype(BF16)
        pair_sum.wait_send()

    @pl.when(jnp.logical_not(final_here))
    def _():
        cross_sum.start()
        pair_sum.wait_recv()
        cross_sum.wait_recv()
        out[...] = (o3_in[0].astype(F32) + o3_in[1].astype(F32)).astype(BF16)
        cross_sum.wait_send()
        own_sum.wait_send()

    for copy in started:
        copy.wait_send()
    for gather in (q, k, o):
        gather.finish_sends()
    o.end_half(ow)
    for group in range(G):
        @pl.when(4 * group + at.g != h)
        def _(group=group):
            spread_copy(group).wait_send()


def shards(
    tokens,
    raw_keys,
    raw_values,
    query_weight,
    output_weight,
    key_expand,
    key_mix,
    key_reduce,
    value_expand,
    value_mix,
    value_reduce,
):
    vmem = pltpu.VMEM
    dma = pltpu.SemaphoreType.DMA
    ring = [dma((4,)), dma((4,)), dma((2, 3, 4)), dma((2, 3, 4))]
    out = pl.pallas_call(
        kernel,
        out_shape=jax.ShapeDtypeStruct((160, 128), BF16),
        in_specs=[pl.BlockSpec(memory_space=vmem)] * 11,
        out_specs=pl.BlockSpec(memory_space=vmem),
        scratch_shapes=[
            vmem((16, 768), BF16),
            vmem((16, 512), BF16),
            vmem((272, 768), BF16),
            vmem((272, 512), BF16),
            vmem((2, 256, 768), BF16),
            vmem((272, 768), F32),
            vmem((64, 768), F32),
            vmem((G, 48, 128), BF16),
            vmem((4, 48, 128), BF16),
            vmem((4, 640, 384), BF16),
            vmem((2, 640, 512), BF16),
            vmem((2, 4, 1280, 128), BF16),
            vmem((128, 2560), BF16),
            vmem((2, 2, 128, 384), BF16),
            vmem((128, 384), BF16),
            vmem((2, 512, 256), BF16),
            vmem((8, 512, 512), F32),
            vmem((512, 128), F32),
            vmem((4, 128, 128), F32),
            vmem((4, 128, 128), F32),
            vmem((4, 128, 128), F32),
            vmem((4, 128, 128), BF16),
            vmem((4, 8, 128), F32),
            vmem((4, 128, 128), BF16),
            vmem((4, 8, 128), F32),
            vmem((256, 512), BF16),
            vmem((2, 4, 2, 160, 128), F32),
            vmem((2, 4, 2, 160, 128), BF16),
            vmem((2, 4, 160, 128), BF16),
            vmem((2, 4, 160, 128), BF16),
            vmem((2, 3, 160, 128), BF16),
            vmem((2, 160, 128), BF16),
            vmem((2, 160, 128), BF16),
            *ring,
            *ring,
            *ring,
            dma((4,)),
            dma((4,)),
            dma((3, 8)),
            dma((3, 8)),
            dma((14,)),
            dma((14,)),
            dma((2, 5)),
            dma((2, 5)),
        ],
        compiler_params=pltpu.CompilerParams(
            collective_id=0, has_side_effects=True, vmem_limit_bytes=56 * 1024 * 1024
        ),
        name="branch",
    )(
        tokens,
        raw_keys,
        raw_values,
        query_weight,
        output_weight.T,
        key_expand,
        key_mix,
        key_reduce.T,
        value_expand,
        value_mix,
        value_reduce,
    )
    return out.T


def solution(mesh):
    in_specs = (
        P("seq", None),
        P(SEQ_HEAD, None),
        P(SEQ_HEAD, None),
        P("seq", "head"),
        P("head", "seq"),
        P(),
        P(),
        P(),
        P(),
        P(),
        P(),
    )
    return jax.shard_map(
        shards, mesh=mesh, in_specs=in_specs, out_specs=P("seq", "head"), check_vma=False
    )
```

```python
import jax
import jax.numpy as jnp
from jax import lax
from jax.experimental import pallas as pl
from jax.experimental.pallas import tpu as pltpu
from jax.sharding import PartitionSpec as P

G = 4
BLK = 32
STRIDE = 16
CTX = 126976
DK = 192
DV = 128
SEQ_HEAD = ("seq", "head")
MESH = pl.DeviceIdType.MESH
BF16 = jnp.bfloat16
F32 = jnp.float32
EXP2_SCALE = DK**-0.5 * 1.4426950408889634


def compress_part(
    raw, edge, has_next, expands, starts, mix, reduce_weight, reduce_dim, order, moved, projected, hidden
):
    moved[0:256, :] = jnp.dot(order, raw[...], preferred_element_type=F32).astype(BF16)
    moved[256:272, :] = jnp.where(has_next, edge[...], jnp.zeros_like(edge))
    row = lax.broadcasted_iota(jnp.int32, (16, 768), 0)
    for group in range(G):
        expand = expands[group]
        start = starts[group]
        projected[...] = jnp.dot(
            moved[:, start : start + expand.shape[0]], expand, preferred_element_type=F32
        )
        first = jnp.zeros((16, 768), F32)
        second = jnp.zeros((16, 768), F32)
        for p in range(STRIDE):
            block = projected[16 * p : 16 * p + 16, :]
            first = first + block * mix[p : p + 1, :]
            second = second + block * mix[STRIDE + p : STRIDE + p + 1, :]
        beyond = jnp.sum(projected[256:272, :] * mix[STRIDE:, :], axis=0, keepdims=True)
        later = jnp.where(row == 15, beyond, pltpu.roll(second, 15, 0))
        hidden[16 * group : 16 * group + 16, :] = first + later
    value = hidden[...]
    activated = (0.5 * value * (1.0 + lax.erf(value * 0.5**0.5))).astype(BF16)
    return lax.dot_general(
        activated, reduce_weight[...], (((1,), (reduce_dim,)), ((), ())), preferred_element_type=F32
    ).astype(BF16)


class Place:
    def __init__(self):
        self.s = s = lax.axis_index("seq")
        self.h = h = lax.axis_index("head")
        self.y, self.z = s // 8, s % 8
        self.g, self.j = h // 4, h % 4
        self.core = h % 2
        self.x = (h // 2) % 4
        self.y_hi = h // 8
        self.parity = self.y % 2
        self.seq_pair = (self.y + 1 - 2 * self.parity) * 8 + self.z
        self.mate = h + 1 - 2 * self.core
        self.head_pair = h + 2 - 4 * ((h // 2) % 2)
        self.head_far = (h + 8) % 16
        self.right = self.y * 8 + (self.z + 1) % 8
        self.left = self.y * 8 + (self.z + 7) % 8

    def seq_at(self, y):
        return y * 8 + self.z


def remote(src, dst, send_sem, recv_sem, seq, head):
    return pltpu.make_async_remote_copy(
        src_ref=src,
        dst_ref=dst,
        send_sem=send_sem,
        recv_sem=recv_sem,
        device_id=(seq, head),
        device_id_type=MESH,
    )


class Gather:
    def __init__(self, at, buf, rows, streams, sems):
        self.at, self.buf, self.rows, self.streams = at, buf, rows, streams
        self.ys, self.yr, self.zs, self.zr = sems
        self.started = []

    def piece(self, i, z):
        start = pl.multiple_of(self.rows * z, 16)
        return self.buf.at[i, pl.ds(start, self.rows), :]

    def block(self, stream, z):
        first, count, _ = self.streams[stream]
        start = pl.multiple_of(self.rows * z, 16)
        return self.buf.at[pl.ds(first, count), pl.ds(start, self.rows), :]

    def y_copy(self, i, source):
        at = self.at
        target = (at.y + 4 - i) % 4
        return remote(
            source(target), self.piece(i, at.z), self.ys.at[i], self.yr.at[i], at.seq_at(target), at.h
        )

    def start_y(self, source):
        for i in (1, 2, 3):
            copy = self.y_copy(i, source)
            copy.start()
            self.started.append(copy)

    def first_z(self, source, streams):
        for stream in streams:
            first, count, _ = self.streams[stream]
            for i in range(first, first + count):
                if i > 0:
                    self.y_copy(i, source).wait_recv()
            self.send_z(stream, 1)

    def z_copy(self, way, stream, step, z):
        at = self.at
        block = self.block(stream, z)
        return remote(
            block,
            block,
            self.zs.at[way, stream, step - 1],
            self.zr.at[way, stream, step - 1],
            (at.right, at.left)[way],
            at.h,
        )

    def ways(self, stream, step):
        return (0, 1) if step < 4 else (self.streams[stream][2],)

    def send_z(self, stream, step):
        at = self.at
        for way in self.ways(stream, step):
            z = (at.z + 8 - (step - 1)) % 8 if way == 0 else (at.z + step - 1) % 8
            copy = self.z_copy(way, stream, step, z)
            copy.start()
            self.started.append(copy)

    def came_from(self, way, step):
        at = self.at
        return (at.z + 8 - step) % 8 if way == 0 else (at.z + step) % 8

    def wait_z(self, stream, step):
        for way in self.ways(stream, step):
            self.z_copy(way, stream, step, self.came_from(way, step)).wait_recv()

    def next_z(self, step):
        for stream in range(len(self.streams)):
            self.wait_z(stream, step - 1)
            self.send_z(stream, step)

    def end_z(self):
        for stream in range(len(self.streams)):
            self.wait_z(stream, 4)

    def finish_sends(self):
        for copy in self.started:
            copy.wait_send()


class HalfGather(Gather):
    def half_copy(self, n, source):
        at = self.at
        i = at.y % 2
        target = at.y // 2 + 2 * n
        return target, remote(
            source, self.piece(i, at.z), self.ys.at[n], self.yr.at[i], at.seq_at(target), at.h
        )

    def start_half(self, source):
        at = self.at
        for n in range(2):
            target, copy = self.half_copy(n, source)

            @pl.when(target != at.y)
            def _(copy=copy):
                copy.start()

            @pl.when(target == at.y)
            def _():
                start = pl.multiple_of(self.rows * at.z, 16)
                self.buf[at.y % 2, pl.ds(start, self.rows), :] = source[...]

    def wait_half(self, i, source):
        at = self.at
        origin = 2 * at.parity + i

        @pl.when(origin != at.y)
        def _():
            remote(
                source, self.piece(i, at.z), self.ys.at[i], self.yr.at[i], at.seq_at(origin), at.h
            ).wait_recv()

    def end_half(self, source):
        for n in range(2):
            target, copy = self.half_copy(n, source)

            @pl.when(target != self.at.y)
            def _(copy=copy):
                copy.wait_send()


QUARTERS = ((0, 1, 0), (1, 2, 1), (3, 1, 0))
HALVES = ((0, 1, 0), (1, 1, 1))


def attend_half(who, at, qbuf, stacked, kvb, scores, lane_max, store, hooks):
    for half in range(2):
        for head in range(2):
            rows = pl.ds((2 * half + head) * 128, 128)
            queries = qbuf[who, half, :, head * DK : (head + 1) * DK]
            stacked[0, rows, 0:DK] = queries
            stacked[1, rows, 0:128] = queries[:, 0:128]
            stacked[1, rows, DK:256] = queries[:, 128:DK]
    last = (3 + 4 - at.y) % 4
    first_position = CTX + at.s * 128
    half_index = (at.h // 2) % 2

    def entry(n):
        return (at.core + n // 4) % 2, (last + n % 4) % 4

    def rows_of(n, start):
        quarter, i = entry(n)
        return kvb[quarter, i].reshape(8, 160, 128)[:, start : start + 32].reshape(256, 128)

    def score_chunk(n, masked):
        quarter, _ = entry(n)
        upper = rows_of(n, 128)
        parts = []
        for side in range(2):
            keys = jnp.concatenate([rows_of(n, 32 * side), upper], axis=1)
            block = lax.dot_general(
                stacked[side], keys, (((1,), (1,)), ((), ())), preferred_element_type=F32
            )
            parts.append(block[:, 0:128])
            tail = block[:, 128:256]
            if masked:
                column = lax.broadcasted_iota(jnp.int32, (512, 128), 1)
                row = lax.broadcasted_iota(jnp.int32, (512, 128), 0) % 128
                ids = 256 * (28 + column // 32) + 64 * (2 * half_index + quarter)
                ids = ids + 32 * side + column % 32
                visible = STRIDE * ids + BLK - 1 <= first_position + row
                tail = jnp.where(visible, tail, -jnp.inf)
            parts.append(tail)
        for k in range(4):
            scores[n, :, 128 * k : 128 * (k + 1)] = parts[k]
        return jnp.maximum(jnp.maximum(parts[0], parts[1]), jnp.maximum(parts[2], parts[3]))

    lane_max[...] = score_chunk(0, True)
    for n in (1, 2, 3):
        lane_max[...] = jnp.maximum(lane_max[...], score_chunk(n, False))
    hooks[0]()
    lane_max[...] = jnp.maximum(lane_max[...], score_chunk(4, True))
    for n in (5, 6, 7):
        lane_max[...] = jnp.maximum(lane_max[...], score_chunk(n, False))
    hooks[1]()

    for head in range(4):
        rows = slice(head * 128, (head + 1) * 128)
        row_max = jnp.max(lane_max[rows, :], axis=1, keepdims=True)
        total = jnp.zeros((128, 128), F32)
        numerator = jnp.zeros((128, 128), F32)
        for n in range(8):
            exponent = jnp.exp2((scores[n, rows, :] - row_max) * EXP2_SCALE)
            for k in range(4):
                total = total + exponent[:, 128 * k : 128 * (k + 1)]
            values = jnp.concatenate([rows_of(n, 64), rows_of(n, 96)], axis=0)
            numerator = numerator + jnp.dot(
                exponent.astype(BF16), values, preferred_element_type=F32
            )
        store(head, row_max, jnp.sum(total, axis=1, keepdims=True), numerator)


def branch(
    tokens,
    raw_keys,
    raw_values,
    qw,
    ow,
    key_expand,
    key_mix,
    key_reduce,
    value_expand,
    value_mix,
    value_reduce,
    out,
    edge_keys,
    edge_values,
    moved_keys,
    moved_values,
    placed_expand,
    projected,
    hidden,
    kv4,
    kvt,
    qwb,
    owb,
    kvb,
    tokp,
    qbuf,
    qother,
    stacked,
    scores,
    lane_max,
    mine,
    mine_max,
    mine_total,
    part,
    stats,
    part_in,
    stats_in,
    attended,
    summed,
    o1,
    o1_in,
    o2,
    o2_in,
    o3,
    o3_in,
    q_ys, q_yr, q_zs, q_zr,
    k_ys, k_yr, k_zs, k_zr,
    o_ys, o_yr, o_zs, o_zr,
    r_s, r_r,
    m_s, m_r,
    e_s, e_r,
    t_s, t_r,
    p_s, p_r,
    loads,
):
    at = Place()
    s, h, c = at.s, at.h, at.core

    for copy in loads:
        copy.start()
    barrier = pltpu.get_barrier_semaphore()
    partners = [(s, (h + d) % 16) for d in range(1, 16)]
    partners += [(at.seq_at((at.y + d) % 4), h) for d in (1, 2, 3)]
    partners += [(at.right, h), (at.left, h)]
    partners += [(at.seq_pair, at.head_pair), (at.seq_pair, at.head_far)]
    flat = 16 * s + h
    before, after = (flat + 511) % 512, (flat + 1) % 512
    partners += [(before // 16, before % 16), (after // 16, after % 16)]
    for partner in partners:
        pl.semaphore_signal(barrier, inc=1, device_id=partner, device_id_type=MESH)
    pl.semaphore_wait(barrier, len(partners))
    for copy in loads:
        copy.wait()

    started = []

    def go(copy):
        copy.start()
        started.append(copy)
        return copy

    q = Gather(at, qwb, 80, QUARTERS, (q_ys, q_yr, q_zs, q_zr))
    o = HalfGather(at, owb, 80, HALVES, (o_ys, o_yr, o_zs, o_zr))
    k = Gather(at, kvb.at[c], 160, QUARTERS, (k_ys, k_yr, k_zs, k_zr))

    edge_in = [
        remote(source.at[0:16], target, e_s.at[i], e_r.at[i], before // 16, before % 16)
        for i, (source, target) in enumerate(((raw_keys, edge_keys), (raw_values, edge_values)), 11)
    ]
    for copy in edge_in:
        go(copy)

    def q_source(target):
        return qw.at[:, pl.ds(pl.multiple_of(384 * (target % 2), 128), 384)]

    qwb[0, pl.ds(pl.multiple_of(80 * at.z, 16), 80), :] = qw[
        :, pl.ds(pl.multiple_of(384 * at.parity, 128), 384)
    ]
    q.start_y(q_source)
    q.first_z(q_source, (0,))
    placed_expand[0, 0:DK, :] = key_expand[...]
    placed_expand[0, DK:256, :] = jnp.zeros((256 - DK, 768), BF16)
    placed_expand[1, 0 : 256 - DK, :] = jnp.zeros((256 - DK, 768), BF16)
    placed_expand[1, 256 - DK :, :] = key_expand[...]
    stacked[0, :, DK:] = jnp.zeros((512, 256 - DK), BF16)
    stacked[1, :, 128:DK] = jnp.zeros((512, DK - 128), BF16)

    q.first_z(q_source, (1, 2))

    row = lax.broadcasted_iota(jnp.int32, (256, 256), 0)
    column = lax.broadcasted_iota(jnp.int32, (256, 256), 1)
    order = (column == 16 * (row % 16) + row // 16).astype(F32).astype(BF16)
    for copy in edge_in:
        copy.wait_recv()
    has_next = flat < 511
    packed_keys = compress_part(
        raw_keys,
        edge_keys,
        has_next,
        [placed_expand[group % 2] for group in range(G)],
        (0, 128, 384, 512),
        key_mix,
        key_reduce,
        1,
        order,
        moved_keys,
        projected,
        hidden,
    )
    packed_values = compress_part(
        raw_values,
        edge_values,
        has_next,
        [value_expand[...]] * G,
        (0, 128, 256, 384),
        value_mix,
        value_reduce,
        0,
        order,
        moved_values,
        projected,
        hidden,
    )
    for group in range(G):
        rows = slice(16 * group, 16 * group + 16)
        kv4[group, 0:16, :] = packed_keys[rows, 0:128]
        kv4[group, 16:32, :] = packed_values[rows, :]
        kv4[group, 32:48, 0:64] = packed_keys[rows, 128:DK]
        kv4[group, 32:48, 64:128] = packed_keys[rows, 128:DK]

    def spread_copy(group):
        return remote(kv4.at[group], kvt.at[at.j], r_s.at[group], r_r.at[at.j], s, 4 * group + at.g)

    for group in range(G):
        @pl.when(4 * group + at.g != h)
        def _(group=group):
            spread_copy(group).start()

        @pl.when(4 * group + at.g == h)
        def _(group=group):
            kvt[at.j] = kv4[group]

    def k_source(target):
        return k.piece(0, at.z)

    def mate_copy(quarter, stream, index, z):
        first, count, _ = QUARTERS[stream]
        start = pl.multiple_of(160 * z, 16)
        block = kvb.at[quarter, pl.ds(first, count), pl.ds(start, 160), :]
        return remote(
            block, block, m_s.at[stream, index], m_r.at[stream, index], s, at.mate
        )

    def k_arrived(stream, step):
        k.wait_z(stream, step)
        for way in k.ways(stream, step):
            index = 7 if step == 4 else 3 * way + step
            go(mate_copy(c, stream, index, k.came_from(way, step)))

    def k_round(step):
        for stream in (0, 1, 2):
            k_arrived(stream, step - 1)
            k.send_z(stream, step)

    q.next_z(2)
    for m in range(4):
        @pl.when(4 * at.j + m != h)
        def _(m=m):
            remote(
                kv4.at[0], kvt.at[m], r_s.at[0], r_r.at[m], s, 4 * at.j + m
            ).wait_recv()
    piece = pl.multiple_of(160 * at.z, 16)
    left_lanes = lax.broadcasted_iota(jnp.int32, (16, 128), 1) < 64
    for m in range(4):
        kvb[c, 0, pl.ds(piece + 16 * m, 16), :] = kvt[m, 0:16, :]
        kvb[c, 0, pl.ds(piece + 64 + 16 * m, 16), :] = kvt[m, 16:32, :]
    for m in range(2):
        both = jnp.where(
            left_lanes, kvt[m, 32:48, :].astype(F32), kvt[m + 2, 32:48, :].astype(F32)
        )
        kvb[c, 0, pl.ds(piece + 128 + 16 * m, 16), :] = both.astype(BF16)
    k.start_y(k_source)
    half_tokens = pl.ds(pl.multiple_of(1280 * c, 128), 1280)
    tok_copy = go(
        remote(
            tokens.at[:, half_tokens], tokp.at[:, half_tokens], e_s.at[0], e_r.at[0], at.seq_pair, h
        )
    )
    o.start_half(ow)
    k.first_z(k_source, (0,))
    go(mate_copy(c, 0, 0, at.z))
    q.next_z(3)
    for stream in (1, 2):
        k.first_z(k_source, (stream,))
        go(mate_copy(c, stream, 0, at.z))
    q.next_z(4)
    k_round(2)
    tok_copy.wait_recv()
    arrived_tokens = tokp.at[:, half_tokens]
    go(remote(arrived_tokens, arrived_tokens, e_s.at[13], e_r.at[13], s, at.mate))
    q.end_z()
    other_half = tokp.at[:, pl.ds(pl.multiple_of(1280 - 1280 * c, 128), 1280)]
    remote(other_half, other_half, e_s.at[13], e_r.at[13], s, at.mate).wait_recv()

    def project_queries(source):
        total = jnp.zeros((128, 384), F32)
        for i in range(4):
            start = pl.multiple_of(640 * ((at.y + i) % 4), 128)
            total = total + jnp.dot(
                source[:, pl.ds(start, 640)], qwb[i], preferred_element_type=F32
            )
        return total.astype(BF16)

    qother[...] = project_queries(tokp)
    q_in = [
        remote(qother, qbuf.at[0, at.parity], e_s.at[1], e_r.at[1], at.seq_pair, h),
        remote(qother, qbuf.at[1, at.parity], e_s.at[2], e_r.at[2], at.seq_pair, at.head_pair),
    ]
    go(q_in[0])
    go(q_in[1])
    qbuf[0, at.parity] = project_queries(tokens)
    q_in.append(
        go(
            remote(
                qbuf.at[0, at.parity], qbuf.at[1, at.parity], e_s.at[3], e_r.at[3], s, at.head_pair
            )
        )
    )
    k_round(3)
    for i in (0, 1):
        o.wait_half(i, ow)
        o.send_z(i, 1)
    k_round(4)
    o.next_z(2)
    for stream in (0, 1, 2):
        k_arrived(stream, 4)
    q_in[0].wait_recv()
    q_in[2].wait_recv()
    q_in[1].wait_recv()
    def mate_arrived():
        for stream in (0, 1, 2):
            mate_copy(1 - c, stream, 0, at.z).wait_recv()
            for step in (1, 2, 3, 4):
                for way in k.ways(stream, step):
                    index = 7 if step == 4 else 3 * way + step
                    mate_copy(1 - c, stream, index, k.came_from(way, step)).wait_recv()

    def nothing():
        pass

    lane = lax.broadcasted_iota(jnp.int32, (128, 128), 1)

    part_copies = [
        [
            remote(
                source.at[head], target.at[head], p_s.at[i, head], p_r.at[i, head], s, at.head_pair
            )
            for i, (source, target) in enumerate(((part, part_in), (stats, stats_in)))
        ]
        for head in range(4)
    ]

    def store_part(head, row_max, row_total, numerator):
        part[head] = numerator.astype(BF16)
        tile = jnp.where(lane == 0, row_max, jnp.where(lane == 1, row_total, 0.0))
        stats[head] = jnp.transpose(tile)[0:8, :]
        for copy in part_copies[head]:
            go(copy)

    attend_half(1, at, qbuf, stacked, kvb, scores, lane_max, store_part, (mate_arrived, lambda: o.next_z(3)))
    def store_mine(head, row_max, row_total, numerator):
        mine[head] = numerator
        mine_max[head] = jnp.broadcast_to(row_max, (128, 128))
        mine_total[head] = jnp.broadcast_to(row_total, (128, 128))

    attend_half(0, at, qbuf, stacked, kvb, scores, lane_max, store_mine, (nothing, lambda: o.next_z(4)))
    for head in range(4):
        for copy in part_copies[head]:
            copy.wait_recv()
        tile = jnp.concatenate([stats_in[head], jnp.zeros((120, 128), F32)], axis=0)
        tile = jnp.transpose(tile)
        other_max = jnp.broadcast_to(tile[:, 0:1], (128, 128))
        other_total = jnp.broadcast_to(tile[:, 1:2], (128, 128))
        top = jnp.maximum(mine_max[head], other_max)
        own_part = jnp.exp2((mine_max[head] - top) * EXP2_SCALE)
        other_part = jnp.exp2((other_max - top) * EXP2_SCALE)
        total = mine_total[head] * own_part + other_total * other_part
        value = mine[head] * own_part + part_in[head].astype(F32) * other_part
        attended[0:128, head * DV : (head + 1) * DV] = (value / total).astype(BF16)
    attended_copy = go(
        remote(
            attended.at[0:128], attended.at[128:256], e_s.at[6], e_r.at[6], at.seq_pair, h
        )
    )
    o.end_z()

    mate_sums = []
    for n in range(2):
        if n == 1:
            attended_copy.wait_recv()
        for i in range(2):
            block = lax.dot_general(
                owb[i],
                attended[128 * n : 128 * (n + 1)],
                (((1,), (1,)), ((), ())),
                preferred_element_type=F32,
            ).reshape(2, 2, 160, 128)
            summed[n, 2 * i : 2 * i + 2] = block
            o1[n, 2 * i : 2 * i + 2] = block.astype(BF16)
        mate_sums.append(
            go(remote(o1.at[n, :, 1 - c], o1_in.at[n], t_s.at[n, 0], t_r.at[n, 0], s, at.mate))
        )
    x_sums = [[], []]
    for n in range(2):
        mate_sums[n].wait_recv()
        for x in range(4):
            summed[n, x, 0] = summed[n, x, c] + o1_in[n, x].astype(F32)
            o2[n, x] = summed[n, x, 0].astype(BF16)
        for d in (1, 2, 3):
            x = (at.x + d) % 4
            target = 8 * at.y_hi + 2 * x + c
            x_sums[n].append(
                go(remote(o2.at[n, x], o2_in.at[n, d - 1], t_s.at[n, d], t_r.at[n, d], s, target))
            )

    def x_total(n):
        for copy in x_sums[n]:
            copy.wait_recv()
        value = summed[n, at.x, 0]
        for d in range(3):
            value = value + o2_in[n, d].astype(F32)
        return value

    final_here = at.y_hi == at.parity
    own_sum = remote(o3.at[0], o3_in.at[1], t_s.at[0, 4], t_r.at[0, 4], s, at.head_far)
    cross_sum = remote(o3.at[1], o3_in.at[1], t_s.at[1, 4], t_r.at[0, 4], at.seq_pair, at.head_far)
    pair_sum = remote(o3.at[1], o3_in.at[0], t_s.at[1, 4], t_r.at[1, 4], at.seq_pair, h)
    own = x_total(0)
    o3[0] = own.astype(BF16)

    @pl.when(jnp.logical_not(final_here))
    def _():
        own_sum.start()

    o3[1] = x_total(1).astype(BF16)

    @pl.when(final_here)
    def _():
        pair_sum.start()
        own_sum.wait_recv()
        out[...] = (own + o3_in[1].astype(F32)).astype(BF16)
        pair_sum.wait_send()

    @pl.when(jnp.logical_not(final_here))
    def _():
        cross_sum.start()
        pair_sum.wait_recv()
        cross_sum.wait_recv()
        out[...] = (o3_in[0].astype(F32) + o3_in[1].astype(F32)).astype(BF16)
        cross_sum.wait_send()
        own_sum.wait_send()

    for copy in started:
        copy.wait_send()
    for gather in (q, k, o):
        gather.finish_sends()
    o.end_half(ow)
    for group in range(G):
        @pl.when(4 * group + at.g != h)
        def _(group=group):
            spread_copy(group).wait_send()


def kernel(*refs):
    operands, out, local, scratch = refs[:11], refs[11], refs[12:23], refs[23:-1]
    order = (3, 1, 2, 0, 4, 5, 6, 8, 9, 7, 10)
    loads = [pltpu.make_async_copy(operands[i], local[i], refs[-1].at[i]) for i in order]
    branch(*local, out, *scratch, loads)


def shards(
    tokens,
    raw_keys,
    raw_values,
    query_weight,
    output_weight,
    key_expand,
    key_mix,
    key_reduce,
    value_expand,
    value_mix,
    value_reduce,
):
    vmem = pltpu.VMEM
    dma = pltpu.SemaphoreType.DMA
    ring = [dma((4,)), dma((4,)), dma((2, 3, 4)), dma((2, 3, 4))]
    operands = (
        tokens,
        raw_keys,
        raw_values,
        query_weight,
        output_weight.T,
        key_expand,
        key_mix,
        key_reduce.T,
        value_expand,
        value_mix,
        value_reduce,
    )
    out = pl.pallas_call(
        kernel,
        out_shape=jax.ShapeDtypeStruct((160, 128), BF16),
        in_specs=[pl.BlockSpec(memory_space=pltpu.HBM)] * 11,
        out_specs=pl.BlockSpec(memory_space=vmem),
        scratch_shapes=[
            *[vmem(operand.shape, operand.dtype) for operand in operands],
            vmem((16, 768), BF16),
            vmem((16, 512), BF16),
            vmem((272, 768), BF16),
            vmem((272, 512), BF16),
            vmem((2, 256, 768), BF16),
            vmem((272, 768), F32),
            vmem((64, 768), F32),
            vmem((G, 48, 128), BF16),
            vmem((4, 48, 128), BF16),
            vmem((4, 640, 384), BF16),
            vmem((2, 640, 512), BF16),
            vmem((2, 4, 1280, 128), BF16),
            vmem((128, 2560), BF16),
            vmem((2, 2, 128, 384), BF16),
            vmem((128, 384), BF16),
            vmem((2, 512, 256), BF16),
            vmem((8, 512, 512), F32),
            vmem((512, 128), F32),
            vmem((4, 128, 128), F32),
            vmem((4, 128, 128), F32),
            vmem((4, 128, 128), F32),
            vmem((4, 128, 128), BF16),
            vmem((4, 8, 128), F32),
            vmem((4, 128, 128), BF16),
            vmem((4, 8, 128), F32),
            vmem((256, 512), BF16),
            vmem((2, 4, 2, 160, 128), F32),
            vmem((2, 4, 2, 160, 128), BF16),
            vmem((2, 4, 160, 128), BF16),
            vmem((2, 4, 160, 128), BF16),
            vmem((2, 3, 160, 128), BF16),
            vmem((2, 160, 128), BF16),
            vmem((2, 160, 128), BF16),
            *ring,
            *ring,
            *ring,
            dma((4,)),
            dma((4,)),
            dma((3, 8)),
            dma((3, 8)),
            dma((14,)),
            dma((14,)),
            dma((2, 5)),
            dma((2, 5)),
            dma((2, 4)),
            dma((2, 4)),
            dma((11,)),
        ],
        compiler_params=pltpu.CompilerParams(
            collective_id=0, has_side_effects=True, vmem_limit_bytes=56 * 1024 * 1024
        ),
        name="branch",
    )(*operands)
    return out.T


def solution(mesh):
    in_specs = (
        P("seq", None),
        P(SEQ_HEAD, None),
        P(SEQ_HEAD, None),
        P("seq", "head"),
        P("head", "seq"),
        P(),
        P(),
        P(),
        P(),
        P(),
        P(),
    )
    return jax.shard_map(
        shards, mesh=mesh, in_specs=in_specs, out_specs=P("seq", "head"), check_vma=False
    )
```

```python
import jax
import jax.numpy as jnp
from jax import lax
from jax.experimental import pallas as pl
from jax.experimental.pallas import tpu as pltpu
from jax.sharding import PartitionSpec as P

G = 4
BLK = 32
STRIDE = 16
CTX = 126976
DK = 192
DV = 128
SEQ_HEAD = ("seq", "head")
MESH = pl.DeviceIdType.MESH
BF16 = jnp.bfloat16
F32 = jnp.float32
EXP2_SCALE = DK**-0.5 * 1.4426950408889634


def compress_part(
    raw, edge, has_next, expands, starts, mix, reduce_weight, reduce_dim, order, moved, projected, hidden
):
    moved[0:256, :] = jnp.dot(order, raw[...], preferred_element_type=F32).astype(BF16)
    moved[256:272, :] = jnp.where(has_next, edge[...], jnp.zeros_like(edge))
    row = lax.broadcasted_iota(jnp.int32, (16, 768), 0)
    for group in range(G):
        expand = expands[group]
        start = starts[group]
        projected[...] = jnp.dot(
            moved[:, start : start + expand.shape[0]], expand, preferred_element_type=F32
        )
        first = jnp.zeros((16, 768), F32)
        second = jnp.zeros((16, 768), F32)
        for p in range(STRIDE):
            block = projected[16 * p : 16 * p + 16, :]
            first = first + block * mix[p : p + 1, :]
            second = second + block * mix[STRIDE + p : STRIDE + p + 1, :]
        beyond = jnp.sum(projected[256:272, :] * mix[STRIDE:, :], axis=0, keepdims=True)
        later = jnp.where(row == 15, beyond, pltpu.roll(second, 15, 0))
        hidden[16 * group : 16 * group + 16, :] = first + later
    value = hidden[...]
    activated = (0.5 * value * (1.0 + lax.erf(value * 0.5**0.5))).astype(BF16)
    return lax.dot_general(
        activated, reduce_weight[...], (((1,), (reduce_dim,)), ((), ())), preferred_element_type=F32
    ).astype(BF16)


class Place:
    def __init__(self):
        self.s = s = lax.axis_index("seq")
        self.h = h = lax.axis_index("head")
        self.y, self.z = s // 8, s % 8
        self.g, self.j = h // 4, h % 4
        self.core = h % 2
        self.x = (h // 2) % 4
        self.y_hi = h // 8
        self.parity = self.y % 2
        self.seq_pair = (self.y + 1 - 2 * self.parity) * 8 + self.z
        self.mate = h + 1 - 2 * self.core
        self.head_pair = h + 2 - 4 * ((h // 2) % 2)
        self.head_far = (h + 8) % 16
        self.right = self.y * 8 + (self.z + 1) % 8
        self.left = self.y * 8 + (self.z + 7) % 8

    def seq_at(self, y):
        return y * 8 + self.z


def remote(src, dst, send_sem, recv_sem, seq, head):
    return pltpu.make_async_remote_copy(
        src_ref=src,
        dst_ref=dst,
        send_sem=send_sem,
        recv_sem=recv_sem,
        device_id=(seq, head),
        device_id_type=MESH,
    )


class Gather:
    def __init__(self, at, buf, rows, streams, sems):
        self.at, self.buf, self.rows, self.streams = at, buf, rows, streams
        self.ys, self.yr, self.zs, self.zr = sems
        self.started = []

    def piece(self, i, z):
        start = pl.multiple_of(self.rows * z, 16)
        return self.buf.at[i, pl.ds(start, self.rows), :]

    def block(self, stream, z):
        first, count, _ = self.streams[stream]
        start = pl.multiple_of(self.rows * z, 16)
        return self.buf.at[pl.ds(first, count), pl.ds(start, self.rows), :]

    def y_copy(self, i, source):
        at = self.at
        target = (at.y + 4 - i) % 4
        return remote(
            source(target), self.piece(i, at.z), self.ys.at[i], self.yr.at[i], at.seq_at(target), at.h
        )

    def start_y(self, source):
        for i in (1, 2, 3):
            copy = self.y_copy(i, source)
            copy.start()
            self.started.append(copy)

    def first_z(self, source, streams):
        for stream in streams:
            first, count, _ = self.streams[stream]
            for i in range(first, first + count):
                if i > 0:
                    self.y_copy(i, source).wait_recv()
            self.send_z(stream, 1)

    def z_copy(self, way, stream, step, z):
        at = self.at
        block = self.block(stream, z)
        return remote(
            block,
            block,
            self.zs.at[way, stream, step - 1],
            self.zr.at[way, stream, step - 1],
            (at.right, at.left)[way],
            at.h,
        )

    def ways(self, stream, step):
        return (0, 1) if step < 4 else (self.streams[stream][2],)

    def send_z(self, stream, step):
        at = self.at
        for way in self.ways(stream, step):
            z = (at.z + 8 - (step - 1)) % 8 if way == 0 else (at.z + step - 1) % 8
            copy = self.z_copy(way, stream, step, z)
            copy.start()
            self.started.append(copy)

    def came_from(self, way, step):
        at = self.at
        return (at.z + 8 - step) % 8 if way == 0 else (at.z + step) % 8

    def wait_z(self, stream, step):
        for way in self.ways(stream, step):
            self.z_copy(way, stream, step, self.came_from(way, step)).wait_recv()

    def next_z(self, step):
        for stream in range(len(self.streams)):
            self.wait_z(stream, step - 1)
            self.send_z(stream, step)

    def end_z(self):
        for stream in range(len(self.streams)):
            self.wait_z(stream, 4)

    def finish_sends(self):
        for copy in self.started:
            copy.wait_send()


class HalfGather(Gather):
    def half_copy(self, n, source):
        at = self.at
        i = at.y % 2
        target = at.y // 2 + 2 * n
        return target, remote(
            source, self.piece(i, at.z), self.ys.at[n], self.yr.at[i], at.seq_at(target), at.h
        )

    def start_half(self, source):
        at = self.at
        for n in range(2):
            target, copy = self.half_copy(n, source)

            @pl.when(target != at.y)
            def _(copy=copy):
                copy.start()

            @pl.when(target == at.y)
            def _():
                start = pl.multiple_of(self.rows * at.z, 16)
                self.buf[at.y % 2, pl.ds(start, self.rows), :] = source[...]

    def wait_half(self, i, source):
        at = self.at
        origin = 2 * at.parity + i

        @pl.when(origin != at.y)
        def _():
            remote(
                source, self.piece(i, at.z), self.ys.at[i], self.yr.at[i], at.seq_at(origin), at.h
            ).wait_recv()

    def end_half(self, source):
        for n in range(2):
            target, copy = self.half_copy(n, source)

            @pl.when(target != self.at.y)
            def _(copy=copy):
                copy.wait_send()


QUARTERS = ((0, 1, 0), (1, 2, 1), (3, 1, 0))
HALVES = ((0, 1, 0), (1, 1, 1))


def attend_half(who, at, qbuf, stacked, kvb, scores, lane_max, store, hooks):
    for half in range(2):
        for head in range(2):
            rows = pl.ds((2 * half + head) * 128, 128)
            queries = qbuf[who, half, :, head * DK : (head + 1) * DK]
            stacked[0, rows, 0:DK] = queries
            stacked[1, rows, 0:128] = queries[:, 0:128]
            stacked[1, rows, DK:256] = queries[:, 128:DK]
    last = (3 + 4 - at.y) % 4
    first_position = CTX + at.s * 128
    half_index = (at.h // 2) % 2

    def entry(n):
        return (at.core + n // 4) % 2, (last + n % 4) % 4

    def rows_of(n, start):
        quarter, i = entry(n)
        return kvb[quarter, i].reshape(8, 160, 128)[:, start : start + 32].reshape(256, 128)

    def score_chunk(n, masked):
        quarter, _ = entry(n)
        upper = rows_of(n, 128)
        parts = []
        for side in range(2):
            keys = jnp.concatenate([rows_of(n, 32 * side), upper], axis=1)
            block = lax.dot_general(
                stacked[side], keys, (((1,), (1,)), ((), ())), preferred_element_type=F32
            )
            parts.append(block[:, 0:128])
            tail = block[:, 128:256]
            if masked:
                column = lax.broadcasted_iota(jnp.int32, (512, 128), 1)
                row = lax.broadcasted_iota(jnp.int32, (512, 128), 0) % 128
                ids = 256 * (28 + column // 32) + 64 * (2 * half_index + quarter)
                ids = ids + 32 * side + column % 32
                visible = STRIDE * ids + BLK - 1 <= first_position + row
                tail = jnp.where(visible, tail, -jnp.inf)
            parts.append(tail)
        for k in range(4):
            scores[n, :, 128 * k : 128 * (k + 1)] = parts[k]
        return jnp.maximum(jnp.maximum(parts[0], parts[1]), jnp.maximum(parts[2], parts[3]))

    lane_max[...] = score_chunk(0, True)
    for n in (1, 2, 3):
        lane_max[...] = jnp.maximum(lane_max[...], score_chunk(n, False))
    hooks[0]()
    lane_max[...] = jnp.maximum(lane_max[...], score_chunk(4, True))
    for n in (5, 6, 7):
        lane_max[...] = jnp.maximum(lane_max[...], score_chunk(n, False))
    hooks[1]()

    for head in range(4):
        rows = slice(head * 128, (head + 1) * 128)
        row_max = jnp.max(lane_max[rows, :], axis=1, keepdims=True)
        total = jnp.zeros((128, 128), F32)
        numerator = jnp.zeros((128, 128), F32)
        for n in range(8):
            exponent = jnp.exp2((scores[n, rows, :] - row_max) * EXP2_SCALE)
            for k in range(4):
                total = total + exponent[:, 128 * k : 128 * (k + 1)]
            values = jnp.concatenate([rows_of(n, 64), rows_of(n, 96)], axis=0)
            numerator = numerator + jnp.dot(
                exponent.astype(BF16), values, preferred_element_type=F32
            )
        store(head, row_max, jnp.sum(total, axis=1, keepdims=True), numerator)


def branch(
    tokens,
    raw_keys,
    raw_values,
    qw,
    ow,
    key_expand,
    key_mix,
    key_reduce,
    value_expand,
    value_mix,
    value_reduce,
    out,
    edge_keys,
    edge_values,
    moved_keys,
    moved_values,
    placed_expand,
    projected,
    hidden,
    kv4,
    kvt,
    qwb,
    owb,
    kvb,
    tokp,
    qbuf,
    qother,
    stacked,
    scores,
    lane_max,
    mine,
    mine_max,
    mine_total,
    part,
    stats,
    part_in,
    stats_in,
    attended,
    summed,
    o1,
    o1_in,
    o2,
    o2_in,
    o3,
    o3_in,
    q_ys, q_yr, q_zs, q_zr,
    k_ys, k_yr, k_zs, k_zr,
    o_ys, o_yr, o_zs, o_zr,
    r_s, r_r,
    m_s, m_r,
    e_s, e_r,
    t_s, t_r,
    p_s, p_r,
    a_s, a_r,
    loads,
):
    at = Place()
    s, h, c = at.s, at.h, at.core

    for copy in loads:
        copy.start()
    barrier = pltpu.get_barrier_semaphore()
    partners = [(s, (h + d) % 16) for d in range(1, 16)]
    partners += [(at.seq_at((at.y + d) % 4), h) for d in (1, 2, 3)]
    partners += [(at.right, h), (at.left, h)]
    partners += [(at.seq_pair, at.head_pair), (at.seq_pair, at.head_far)]
    flat = 16 * s + h
    before, after = (flat + 511) % 512, (flat + 1) % 512
    partners += [(before // 16, before % 16), (after // 16, after % 16)]
    for partner in partners:
        pl.semaphore_signal(barrier, inc=1, device_id=partner, device_id_type=MESH)
    pl.semaphore_wait(barrier, len(partners))
    for copy in loads:
        copy.wait()

    started = []

    def go(copy):
        copy.start()
        started.append(copy)
        return copy

    q = Gather(at, qwb, 80, QUARTERS, (q_ys, q_yr, q_zs, q_zr))
    o = HalfGather(at, owb, 80, HALVES, (o_ys, o_yr, o_zs, o_zr))
    k = Gather(at, kvb.at[c], 160, QUARTERS, (k_ys, k_yr, k_zs, k_zr))

    edge_in = [
        remote(source.at[0:16], target, e_s.at[i], e_r.at[i], before // 16, before % 16)
        for i, (source, target) in enumerate(((raw_keys, edge_keys), (raw_values, edge_values)), 11)
    ]
    for copy in edge_in:
        go(copy)

    def q_source(target):
        return qw.at[:, pl.ds(pl.multiple_of(384 * (target % 2), 128), 384)]

    qwb[0, pl.ds(pl.multiple_of(80 * at.z, 16), 80), :] = qw[
        :, pl.ds(pl.multiple_of(384 * at.parity, 128), 384)
    ]
    q.start_y(q_source)
    q.first_z(q_source, (0,))
    placed_expand[0, 0:DK, :] = key_expand[...]
    placed_expand[0, DK:256, :] = jnp.zeros((256 - DK, 768), BF16)
    placed_expand[1, 0 : 256 - DK, :] = jnp.zeros((256 - DK, 768), BF16)
    placed_expand[1, 256 - DK :, :] = key_expand[...]
    stacked[0, :, DK:] = jnp.zeros((512, 256 - DK), BF16)
    stacked[1, :, 128:DK] = jnp.zeros((512, DK - 128), BF16)

    q.first_z(q_source, (1, 2))

    row = lax.broadcasted_iota(jnp.int32, (256, 256), 0)
    column = lax.broadcasted_iota(jnp.int32, (256, 256), 1)
    order = (column == 16 * (row % 16) + row // 16).astype(F32).astype(BF16)
    for copy in edge_in:
        copy.wait_recv()
    has_next = flat < 511
    packed_keys = compress_part(
        raw_keys,
        edge_keys,
        has_next,
        [placed_expand[group % 2] for group in range(G)],
        (0, 128, 384, 512),
        key_mix,
        key_reduce,
        1,
        order,
        moved_keys,
        projected,
        hidden,
    )
    packed_values = compress_part(
        raw_values,
        edge_values,
        has_next,
        [value_expand[...]] * G,
        (0, 128, 256, 384),
        value_mix,
        value_reduce,
        0,
        order,
        moved_values,
        projected,
        hidden,
    )
    for group in range(G):
        rows = slice(16 * group, 16 * group + 16)
        kv4[group, 0:16, :] = packed_keys[rows, 0:128]
        kv4[group, 16:32, :] = packed_values[rows, :]
        kv4[group, 32:48, 0:64] = packed_keys[rows, 128:DK]
        kv4[group, 32:48, 64:128] = packed_keys[rows, 128:DK]

    def spread_copy(group):
        return remote(kv4.at[group], kvt.at[at.j], r_s.at[group], r_r.at[at.j], s, 4 * group + at.g)

    for group in range(G):
        @pl.when(4 * group + at.g != h)
        def _(group=group):
            spread_copy(group).start()

        @pl.when(4 * group + at.g == h)
        def _(group=group):
            kvt[at.j] = kv4[group]

    def k_source(target):
        return k.piece(0, at.z)

    def mate_copy(quarter, stream, index, z):
        first, count, _ = QUARTERS[stream]
        start = pl.multiple_of(160 * z, 16)
        block = kvb.at[quarter, pl.ds(first, count), pl.ds(start, 160), :]
        return remote(
            block, block, m_s.at[stream, index], m_r.at[stream, index], s, at.mate
        )

    def k_arrived(stream, step):
        k.wait_z(stream, step)
        for way in k.ways(stream, step):
            index = 7 if step == 4 else 3 * way + step
            go(mate_copy(c, stream, index, k.came_from(way, step)))

    def k_round(step):
        for stream in (0, 1, 2):
            k_arrived(stream, step - 1)
            k.send_z(stream, step)

    q.next_z(2)
    for m in range(4):
        @pl.when(4 * at.j + m != h)
        def _(m=m):
            remote(
                kv4.at[0], kvt.at[m], r_s.at[0], r_r.at[m], s, 4 * at.j + m
            ).wait_recv()
    piece = pl.multiple_of(160 * at.z, 16)
    left_lanes = lax.broadcasted_iota(jnp.int32, (16, 128), 1) < 64
    for m in range(4):
        kvb[c, 0, pl.ds(piece + 16 * m, 16), :] = kvt[m, 0:16, :]
        kvb[c, 0, pl.ds(piece + 64 + 16 * m, 16), :] = kvt[m, 16:32, :]
    for m in range(2):
        both = jnp.where(
            left_lanes, kvt[m, 32:48, :].astype(F32), kvt[m + 2, 32:48, :].astype(F32)
        )
        kvb[c, 0, pl.ds(piece + 128 + 16 * m, 16), :] = both.astype(BF16)
    k.start_y(k_source)
    half_tokens = pl.ds(pl.multiple_of(1280 * c, 128), 1280)
    tok_copy = go(
        remote(
            tokens.at[:, half_tokens], tokp.at[:, half_tokens], e_s.at[0], e_r.at[0], at.seq_pair, h
        )
    )
    o.start_half(ow)
    k.first_z(k_source, (0,))
    go(mate_copy(c, 0, 0, at.z))
    q.next_z(3)
    for stream in (1, 2):
        k.first_z(k_source, (stream,))
        go(mate_copy(c, stream, 0, at.z))
    q.next_z(4)
    k_round(2)
    tok_copy.wait_recv()
    arrived_tokens = tokp.at[:, half_tokens]
    go(remote(arrived_tokens, arrived_tokens, e_s.at[13], e_r.at[13], s, at.mate))
    q.end_z()
    other_half = tokp.at[:, pl.ds(pl.multiple_of(1280 - 1280 * c, 128), 1280)]
    remote(other_half, other_half, e_s.at[13], e_r.at[13], s, at.mate).wait_recv()

    def project_queries(source):
        total = jnp.zeros((128, 384), F32)
        for i in range(4):
            start = pl.multiple_of(640 * ((at.y + i) % 4), 128)
            total = total + jnp.dot(
                source[:, pl.ds(start, 640)], qwb[i], preferred_element_type=F32
            )
        return total.astype(BF16)

    qother[...] = project_queries(tokp)
    q_in = [
        remote(qother, qbuf.at[0, at.parity], e_s.at[1], e_r.at[1], at.seq_pair, h),
        remote(qother, qbuf.at[1, at.parity], e_s.at[2], e_r.at[2], at.seq_pair, at.head_pair),
    ]
    go(q_in[0])
    go(q_in[1])
    qbuf[0, at.parity] = project_queries(tokens)
    q_in.append(
        go(
            remote(
                qbuf.at[0, at.parity], qbuf.at[1, at.parity], e_s.at[3], e_r.at[3], s, at.head_pair
            )
        )
    )
    k_round(3)
    for i in (0, 1):
        o.wait_half(i, ow)
        o.send_z(i, 1)
    k_round(4)
    o.next_z(2)
    for stream in (0, 1, 2):
        k_arrived(stream, 4)
    q_in[0].wait_recv()
    q_in[2].wait_recv()
    q_in[1].wait_recv()
    def mate_arrived():
        for stream in (0, 1, 2):
            mate_copy(1 - c, stream, 0, at.z).wait_recv()
            for step in (1, 2, 3, 4):
                for way in k.ways(stream, step):
                    index = 7 if step == 4 else 3 * way + step
                    mate_copy(1 - c, stream, index, k.came_from(way, step)).wait_recv()

    def nothing():
        pass

    lane = lax.broadcasted_iota(jnp.int32, (128, 128), 1)

    part_copies = [
        [
            remote(
                source.at[head], target.at[head], p_s.at[i, head], p_r.at[i, head], s, at.head_pair
            )
            for i, (source, target) in enumerate(((part, part_in), (stats, stats_in)))
        ]
        for head in range(4)
    ]

    def store_part(head, row_max, row_total, numerator):
        part[head] = numerator.astype(BF16)
        tile = jnp.where(lane == 0, row_max, jnp.where(lane == 1, row_total, 0.0))
        stats[head] = jnp.transpose(tile)[0:8, :]
        for copy in part_copies[head]:
            go(copy)

    attend_half(1, at, qbuf, stacked, kvb, scores, lane_max, store_part, (mate_arrived, lambda: o.next_z(3)))
    def store_mine(head, row_max, row_total, numerator):
        mine[head] = numerator
        mine_max[head] = jnp.broadcast_to(row_max, (128, 128))
        mine_total[head] = jnp.broadcast_to(row_total, (128, 128))

    attend_half(0, at, qbuf, stacked, kvb, scores, lane_max, store_mine, (nothing, lambda: o.next_z(4)))
    attended_copies = []
    for head in range(4):
        for copy in part_copies[head]:
            copy.wait_recv()
        tile = jnp.concatenate([stats_in[head], jnp.zeros((120, 128), F32)], axis=0)
        tile = jnp.transpose(tile)
        other_max = jnp.broadcast_to(tile[:, 0:1], (128, 128))
        other_total = jnp.broadcast_to(tile[:, 1:2], (128, 128))
        top = jnp.maximum(mine_max[head], other_max)
        own_part = jnp.exp2((mine_max[head] - top) * EXP2_SCALE)
        other_part = jnp.exp2((other_max - top) * EXP2_SCALE)
        total = mine_total[head] * own_part + other_total * other_part
        value = mine[head] * own_part + part_in[head].astype(F32) * other_part
        columns = pl.ds(head * DV, DV)
        attended[0:128, columns] = (value / total).astype(BF16)
        attended_copies.append(
            go(
                remote(
                    attended.at[0:128, columns],
                    attended.at[128:256, columns],
                    a_s.at[head],
                    a_r.at[head],
                    at.seq_pair,
                    h,
                )
            )
        )
    o.end_z()

    mate_sums = []
    for n in range(2):
        if n == 1:
            for copy in attended_copies:
                copy.wait_recv()
        for i in range(2):
            block = lax.dot_general(
                owb[i],
                attended[128 * n : 128 * (n + 1)],
                (((1,), (1,)), ((), ())),
                preferred_element_type=F32,
            ).reshape(2, 2, 160, 128)
            summed[n, 2 * i : 2 * i + 2] = block
            o1[n, 2 * i : 2 * i + 2] = block.astype(BF16)
        mate_sums.append(
            go(remote(o1.at[n, :, 1 - c], o1_in.at[n], t_s.at[n, 0], t_r.at[n, 0], s, at.mate))
        )
    x_sums = [[], []]
    for n in range(2):
        mate_sums[n].wait_recv()
        for x in range(4):
            summed[n, x, 0] = summed[n, x, c] + o1_in[n, x].astype(F32)
            o2[n, x] = summed[n, x, 0].astype(BF16)
        for d in (1, 2, 3):
            x = (at.x + d) % 4
            target = 8 * at.y_hi + 2 * x + c
            x_sums[n].append(
                go(remote(o2.at[n, x], o2_in.at[n, d - 1], t_s.at[n, d], t_r.at[n, d], s, target))
            )

    def x_total(n):
        for copy in x_sums[n]:
            copy.wait_recv()
        value = summed[n, at.x, 0]
        for d in range(3):
            value = value + o2_in[n, d].astype(F32)
        return value

    final_here = at.y_hi == at.parity
    own_sum = remote(o3.at[0], o3_in.at[1], t_s.at[0, 4], t_r.at[0, 4], s, at.head_far)
    cross_sum = remote(o3.at[1], o3_in.at[1], t_s.at[1, 4], t_r.at[0, 4], at.seq_pair, at.head_far)
    pair_sum = remote(o3.at[1], o3_in.at[0], t_s.at[1, 4], t_r.at[1, 4], at.seq_pair, h)
    own = x_total(0)
    o3[0] = own.astype(BF16)

    @pl.when(jnp.logical_not(final_here))
    def _():
        own_sum.start()

    o3[1] = x_total(1).astype(BF16)

    @pl.when(final_here)
    def _():
        pair_sum.start()
        own_sum.wait_recv()
        out[...] = (own + o3_in[1].astype(F32)).astype(BF16)
        pair_sum.wait_send()

    @pl.when(jnp.logical_not(final_here))
    def _():
        cross_sum.start()
        pair_sum.wait_recv()
        cross_sum.wait_recv()
        out[...] = (o3_in[0].astype(F32) + o3_in[1].astype(F32)).astype(BF16)
        cross_sum.wait_send()
        own_sum.wait_send()

    for copy in started:
        copy.wait_send()
    for gather in (q, k, o):
        gather.finish_sends()
    o.end_half(ow)
    for group in range(G):
        @pl.when(4 * group + at.g != h)
        def _(group=group):
            spread_copy(group).wait_send()


def kernel(*refs):
    operands, out, local, scratch = refs[:11], refs[11], refs[12:23], refs[23:-1]
    order = (3, 1, 2, 0, 4, 5, 6, 8, 9, 7, 10)
    loads = [pltpu.make_async_copy(operands[i], local[i], refs[-1].at[i]) for i in order]
    branch(*local, out, *scratch, loads)


def shards(
    tokens,
    raw_keys,
    raw_values,
    query_weight,
    output_weight,
    key_expand,
    key_mix,
    key_reduce,
    value_expand,
    value_mix,
    value_reduce,
):
    vmem = pltpu.VMEM
    dma = pltpu.SemaphoreType.DMA
    ring = [dma((4,)), dma((4,)), dma((2, 3, 4)), dma((2, 3, 4))]
    operands = (
        tokens,
        raw_keys,
        raw_values,
        query_weight,
        output_weight.T,
        key_expand,
        key_mix,
        key_reduce.T,
        value_expand,
        value_mix,
        value_reduce,
    )
    out = pl.pallas_call(
        kernel,
        out_shape=jax.ShapeDtypeStruct((160, 128), BF16),
        in_specs=[pl.BlockSpec(memory_space=pltpu.HBM)] * 11,
        out_specs=pl.BlockSpec(memory_space=vmem),
        scratch_shapes=[
            *[vmem(operand.shape, operand.dtype) for operand in operands],
            vmem((16, 768), BF16),
            vmem((16, 512), BF16),
            vmem((272, 768), BF16),
            vmem((272, 512), BF16),
            vmem((2, 256, 768), BF16),
            vmem((272, 768), F32),
            vmem((64, 768), F32),
            vmem((G, 48, 128), BF16),
            vmem((4, 48, 128), BF16),
            vmem((4, 640, 384), BF16),
            vmem((2, 640, 512), BF16),
            vmem((2, 4, 1280, 128), BF16),
            vmem((128, 2560), BF16),
            vmem((2, 2, 128, 384), BF16),
            vmem((128, 384), BF16),
            vmem((2, 512, 256), BF16),
            vmem((8, 512, 512), F32),
            vmem((512, 128), F32),
            vmem((4, 128, 128), F32),
            vmem((4, 128, 128), F32),
            vmem((4, 128, 128), F32),
            vmem((4, 128, 128), BF16),
            vmem((4, 8, 128), F32),
            vmem((4, 128, 128), BF16),
            vmem((4, 8, 128), F32),
            vmem((256, 512), BF16),
            vmem((2, 4, 2, 160, 128), F32),
            vmem((2, 4, 2, 160, 128), BF16),
            vmem((2, 4, 160, 128), BF16),
            vmem((2, 4, 160, 128), BF16),
            vmem((2, 3, 160, 128), BF16),
            vmem((2, 160, 128), BF16),
            vmem((2, 160, 128), BF16),
            *ring,
            *ring,
            *ring,
            dma((4,)),
            dma((4,)),
            dma((3, 8)),
            dma((3, 8)),
            dma((14,)),
            dma((14,)),
            dma((2, 5)),
            dma((2, 5)),
            dma((2, 4)),
            dma((2, 4)),
            dma((4,)),
            dma((4,)),
            dma((11,)),
        ],
        compiler_params=pltpu.CompilerParams(
            collective_id=0, has_side_effects=True, vmem_limit_bytes=56 * 1024 * 1024
        ),
        name="branch",
    )(*operands)
    return out.T


def solution(mesh):
    in_specs = (
        P("seq", None),
        P(SEQ_HEAD, None),
        P(SEQ_HEAD, None),
        P("seq", "head"),
        P("head", "seq"),
        P(),
        P(),
        P(),
        P(),
        P(),
        P(),
    )
    return jax.shard_map(
        shards, mesh=mesh, in_specs=in_specs, out_specs=P("seq", "head"), check_vma=False
    )
```
